512 devices in a mesh: owner: 64 (over z, x, core), rep: 8 (over y).
Axes of the slice: x: 4, y: 8, z: 8, core: 2. Of those that a mesh axis runs over, the one named last changes fastest.
Arguments:
- features: float32 [262144, 256], P(('owner', 'rep')), may hold values from -6 to 6
- group_ids: int32 [262144], P(('owner', 'rep')), may hold values from 0 to 65535, as said below
- survive: int32 [262144], P(('owner', 'rep')), may hold values from 0 to 1
- home_row: int32 [65536], replicated, may hold values from 0 to 65535, as said below
- hot_ids: int32 [256], replicated, may hold values from 0 to 65535, as said below
Outputs:
- group_out: float32 [65536, 256], P(('owner', 'rep'))
- group_count: float32 [65536], P(('owner', 'rep'))
- hot_out: float32 [256, 256], P('rep')
- hot_count: float32 [256], P('rep')
The draws below stay inside these ranges and needn't reach their ends.
Inputs may be any that keep to these rules, and one draw needn't show every extreme that they name: home_row is a permutation of the groups. hot_ids holds 256 different groups. `group_ids`: among the rows of one device, 128 name hot groups, and at most 16 rows name non-hot groups g whose home_row[g] // 1024 is one and the same owner index; on every device some owners get exactly 16 such rows.
All inputs are finite; a program needn't handle non-finite values.
Results may differ from the reference program's by a relative error of at most 0.00007.
Values sent between devices are 32-bit elements; how exact they have to be, the bound alone decides.
A program may use at most 64 MiB of HBM per device.

```python
import jax
import jax.numpy as jnp

F = 256
GROUPS = 65536
HOT = 256
ROWS_DEV = 512
ROWS = 262144
OWN_GROUPS = 1024
CAP = 16
HOT_ROWS = 128
N_OWNER = 64
DEVICES = 512


def shared_tables(key):
    home = jax.random.permutation(jax.random.fold_in(key, 11), GROUPS).astype(jnp.int32)
    inverse = jnp.zeros((GROUPS,), jnp.int32).at[home].set(jnp.arange(GROUPS, dtype=jnp.int32))
    index = jnp.arange(HOT, dtype=jnp.int32)
    hot = inverse[index % N_OWNER * OWN_GROUPS + OWN_GROUPS - 1 - index // N_OWNER]
    return (home, inverse, hot)


def draw_home_row(key, part):
    return shared_tables(key)[0]


def draw_hot_ids(key, part):
    return shared_tables(key)[2]


def row_layout(key):
    home, inverse, hot = shared_tables(key)
    cold_rows = ROWS_DEV - HOT_ROWS
    span = OWN_GROUPS - HOT // N_OWNER
    chosen = jax.random.randint(jax.random.fold_in(key, 31), (), 0, N_OWNER).astype(jnp.int32)

    def one_device(dev_key):
        keys = jax.random.split(dev_key, 6)
        limit = jax.random.randint(keys[0], (HOT_ROWS,), 1, HOT + 1)
        pick = jax.random.randint(keys[1], (HOT_ROWS,), 0, 1 << 20) % limit
        hot_part = hot[pick]
        shuffled = jax.random.permutation(keys[2], N_OWNER).astype(jnp.int32)
        where_chosen = jnp.argmax((shuffled == chosen).astype(jnp.int32)).astype(jnp.int32)
        first = shuffled[0]
        owners = shuffled.at[where_chosen].set(first).at[0].set(chosen)
        owner = owners[jnp.arange(cold_rows, dtype=jnp.int32) // CAP]
        limit_cold = jax.random.randint(keys[3], (cold_rows,), 1, span + 1)
        within = jax.random.randint(keys[4], (cold_rows,), 0, 1 << 20) % limit_cold
        cold_part = inverse[owner * OWN_GROUPS + within]
        ids = jnp.concatenate([hot_part, cold_part]).astype(jnp.int32)
        flagged = jnp.concatenate([jnp.zeros((HOT_ROWS,), jnp.int32), (owner == chosen).astype(jnp.int32)])
        order = jax.random.permutation(keys[5], ROWS_DEV)
        return (ids[order], flagged[order])
    dev_keys = jax.random.split(jax.random.fold_in(key, 23), DEVICES)
    ids, flagged = jax.vmap(one_device)(dev_keys)
    return (ids.astype(jnp.int32), flagged.astype(jnp.int32))


def draw_group_ids(key, part):
    return row_layout(key)[0].reshape(-1).astype(jnp.int32)


def draw_survive(key, part):
    flagged = row_layout(key)[1]
    coin = jax.random.randint(jax.random.fold_in(key, 41), (DEVICES, ROWS_DEV), 0, 2).astype(jnp.int32)
    full_device = jax.random.randint(jax.random.fold_in(key, 43), (DEVICES,), 0, 16) == 0
    alive = jnp.where((flagged == 1) | full_device[:, None], 1, coin)
    return alive.reshape(-1).astype(jnp.int32)


def level_of(own_key, extent, cuts, low, largest):
    def one(axis_at, parts):
        heights = jax.random.uniform(jax.random.fold_in(jax.random.fold_in(own_key, 6), axis_at), (parts,), jnp.float32, low / len(cuts), largest / len(cuts))
        return jnp.repeat(jnp.exp(heights), extent[axis_at] // parts).reshape((-1,) + (1,) * (len(extent) - axis_at - 1))

    level = one(*cuts[0])
    for cut in cuts[1:]:
        level = level * one(*cut)
    return level


def bell_draw(rng, shape, deviation, most, cuts=(), kind=jnp.bfloat16):
    factor_of = level_of(rng, shape, cuts, -0.22, 0.18) if cuts else 1.0
    drawn = jax.random.normal(rng, shape, jnp.float32) * deviation * factor_of
    return jnp.minimum(jnp.maximum(drawn, -most), most).astype(kind)


def setup_inputs(seed: int = 0) -> dict:
    arg_keys = jax.random.split(jax.random.key(seed), 6)
    features = bell_draw(arg_keys[0], (ROWS, F), 1.0, 6.0, ((0, 512),), jnp.float32)
    group_ids = draw_group_ids(jax.random.fold_in(arg_keys[5], 71), 0)
    survive = draw_survive(jax.random.fold_in(arg_keys[5], 71), 0)
    home_row = draw_home_row(jax.random.fold_in(arg_keys[5], 71), 0)
    hot_ids = draw_hot_ids(jax.random.fold_in(arg_keys[5], 71), 0)
    return {"features": features, "group_ids": group_ids, "survive": survive, "home_row": home_row, "hot_ids": hot_ids}


def reference(features, group_ids, survive, home_row, hot_ids):
    weight = jnp.where(survive == 1, 1.0, 0.0).astype(jnp.float32)
    hot_slot = jnp.zeros((GROUPS,), jnp.int32).at[hot_ids].set(jnp.arange(1, HOT + 1, dtype=jnp.int32))
    hot_of_row = hot_slot[group_ids]
    kept = features * weight[:, None]
    cold_target = jnp.where(hot_of_row > 0, GROUPS, home_row[group_ids]).astype(jnp.int32)
    hot_target = jnp.where(hot_of_row > 0, hot_of_row - 1, HOT).astype(jnp.int32)
    cold_sum = jax.ops.segment_sum(kept, cold_target, num_segments=GROUPS + 1)[:GROUPS]
    cold_count = jax.ops.segment_sum(weight, cold_target, num_segments=GROUPS + 1)[:GROUPS]
    hot_sum = jax.ops.segment_sum(kept, hot_target, num_segments=HOT + 1)[:HOT]
    hot_count = jax.ops.segment_sum(weight, hot_target, num_segments=HOT + 1)[:HOT]
    group_out = cold_sum / jnp.sqrt(1.0 + cold_count)[:, None]
    hot_out = hot_sum / jnp.sqrt(1.0 + hot_count)[:, None]
    return (group_out, cold_count, hot_out, hot_count)
```

```python
import functools

import jax
import jax.numpy as jnp
from jax import lax
from jax.experimental import pallas as pl
from jax.experimental.pallas import tpu as pltpu
from jax.sharding import PartitionSpec as P

OWNER_REP = ("owner", "rep")
MESH = pl.DeviceIdType.MESH
LANES = 128
CAP = 16
INNER = 8


def iota(shape, dim):
    return lax.broadcasted_iota(jnp.int32, shape, dim)


def ones_where(mask):
    return jnp.where(mask, 1.0, 0.0)


def two_parts(x):
    high = x.astype(jnp.bfloat16)
    low = (x - high.astype(jnp.float32)).astype(jnp.bfloat16)
    return high, low


def dot(a, b, dims=(((1,), (0,)), ((), ()))):
    return lax.dot_general(a, b, dims, preferred_element_type=jnp.float32)


def folded(x):
    return x[:, :LANES] + x[:, LANES:]


def column(row):
    n = row.shape[1]
    square = jnp.where(iota((n, n), 0) == iota((n, n), 1), row, 0.0)
    return jnp.sum(square, axis=1, keepdims=True)


def diagonal(square):
    n = square.shape[0]
    return jnp.sum(
        jnp.where(iota((n, n), 0) == iota((n, n), 1), square, 0.0), axis=0, keepdims=True
    )


def kernel(
    sizes,
    gid_ref,
    live_ref,
    hot_ref,
    feat_hbm,
    home_hbm,
    gout,
    gcount,
    hout,
    hcount,
    feat,
    home,
    parts,
    bucket,
    rbucket,
    label,
    rlabel,
    wide,
    rhs,
    dense,
    rdense,
    count,
    rcount,
    hpart,
    rhpart,
    hnum,
    rhnum,
    piece,
    rpiece,
    done,
    rdone,
    in_sem,
    send,
    recv,
):
    n_own, n_rep, own_groups, n_hot = sizes
    rows = gid_ref.shape[1]
    per_rep = own_groups // n_rep
    hot_rep = n_hot // n_rep
    n_z = n_own // INNER
    me = lax.axis_index("owner")
    my = lax.axis_index("rep")

    def peer(i):
        m, k = i // n_z, i % n_z
        dz = ((k + 1) // 2) * (1 - 2 * (k % 2))
        z = (me // INNER + dz + n_z) % n_z
        x = ((me % INNER) // 2 + m // 2) % (INNER // 2)
        return z * INNER + x * 2 + (me + m) % 2

    def rep_peer(i):
        step = (i // 2 + 1) * (1 - 2 * (i % 2))
        return (my + step + n_rep) % n_rep

    barrier = pltpu.get_barrier_semaphore()

    @pl.loop(1, n_own)
    def _(i):
        pl.semaphore_signal(barrier, inc=1, device_id=(peer(i), my), device_id_type=MESH)

    @pl.loop(0, n_rep - 1)
    def _(i):
        pl.semaphore_signal(barrier, inc=1, device_id=(me, rep_peer(i)), device_id_type=MESH)

    get_home = pltpu.make_async_copy(home_hbm, home, in_sem.at[0])
    get_feat = pltpu.make_async_copy(feat_hbm, feat, in_sem.at[1])
    get_home.start()
    get_feat.start()

    gid = gid_ref[...]
    live = live_ref[...] == 1
    match = iota((n_hot, n_hot), 0) == iota((n_hot, n_hot), 1)
    hot_ids = jnp.sum(
        jnp.where(match, hot_ref[...].astype(jnp.float32), 0.0), axis=1, keepdims=True
    )
    hits = ones_where(hot_ids == gid.astype(jnp.float32))
    is_hot = jnp.max(hits, axis=0, keepdims=True) > 0.5
    hot_table = jnp.where(live, hits, 0.0).astype(jnp.bfloat16)
    keep = jnp.logical_and(live, jnp.logical_not(is_hot))

    get_home.wait()
    n_hi = home.shape[0]
    digits = jnp.concatenate(
        [
            (home[...] >> 8).astype(jnp.float32).astype(jnp.bfloat16),
            (home[...] & 255).astype(jnp.float32).astype(jnp.bfloat16),
        ],
        axis=1,
    )
    pick = ones_where(iota((n_hi, rows), 0) == (gid >> 7)).astype(jnp.bfloat16)
    found = dot(digits, pick, (((0,), (0,)), ((), ())))
    low = iota((LANES, rows), 0) == (gid & 127)
    d_high = jnp.sum(jnp.where(low, found[:LANES], 0.0), axis=0, keepdims=True)
    d_low = jnp.sum(jnp.where(low, found[LANES:], 0.0), axis=0, keepdims=True)
    dest = (d_high * 256.0 + d_low).astype(jnp.int32)
    owner = dest // own_groups
    local = dest % own_groups + 1
    member = ones_where(jnp.logical_and(iota((n_own, rows), 0) == owner, keep))
    before = ones_where(iota((rows, rows), 0) < iota((rows, rows), 1)).astype(jnp.bfloat16)
    earlier = dot(member.astype(jnp.bfloat16), before)
    pos = jnp.sum(member * earlier, axis=0, keepdims=True).astype(jnp.int32)
    slot = jnp.where(keep, owner * CAP + pos, -1)

    shift = (me % (LANES // CAP)) * CAP
    at = ones_where(iota((LANES, rows), 0) == pos + shift).astype(jnp.bfloat16)
    two = jnp.concatenate(
        [member * (local >> 5).astype(jnp.float32), member * (local & 31).astype(jnp.float32)],
        axis=0,
    ).astype(jnp.bfloat16)
    two = dot(two, at, (((1,), (1,)), ((), ())))
    names = (two[:n_own] * 32.0 + two[n_own:]).astype(jnp.int32)
    label[...] = names.reshape(n_own, 1, LANES)

    get_feat.wait()
    for h in range(2):
        high, lo = two_parts(feat[:, h * LANES : (h + 1) * LANES])
        parts[h, :, :LANES] = high
        parts[h, :, LANES:] = lo

    def pack(h):
        per = LANES // CAP

        @pl.loop(0, n_own // per)
        def _(j):
            chosen = ones_where(iota((LANES, rows), 0) + j * LANES == slot).astype(jnp.bfloat16)
            packed = folded(dot(chosen, parts[h]))
            bucket[h, pl.ds(j * per, per)] = packed.reshape(per, CAP, LANES)

    pack(0)
    for h in range(2):
        part = folded(dot(hot_table, parts[h]))
        hpart[:, :, h * LANES : (h + 1) * LANES] = part.reshape(n_rep, hot_rep, LANES)
    tally = dot(hot_table, jnp.ones((rows, n_hot), jnp.bfloat16))
    hnum[...] = diagonal(tally)

    rlabel[me] = label[me]
    rbucket[0, me] = bucket[0, me]
    rhpart[my] = hpart[my]
    rhnum[my] = hnum[...]

    pl.semaphore_wait(barrier, n_own - 1 + n_rep - 1)

    def to_owner(src, dst, which, i_peer):
        pltpu.make_async_remote_copy(
            src_ref=src,
            dst_ref=dst,
            send_sem=send.at[which],
            recv_sem=recv.at[which],
            device_id=(i_peer, my),
            device_id_type=MESH,
        ).start()

    def to_rep(src, dst, which, i_peer):
        pltpu.make_async_remote_copy(
            src_ref=src,
            dst_ref=dst,
            send_sem=send.at[which],
            recv_sem=recv.at[which],
            device_id=(me, i_peer),
            device_id_type=MESH,
        ).start()

    def arrived(ref, which, n):
        pltpu.make_async_copy(ref.at[pl.ds(0, n)], ref.at[pl.ds(0, n)], recv.at[which]).wait()

    def left(ref, which, n):
        pltpu.make_async_copy(ref.at[pl.ds(0, n)], ref.at[pl.ds(0, n)], send.at[which]).wait()

    @pl.loop(0, n_rep - 1)
    def _(i):
        o = rep_peer(i)
        to_rep(hpart.at[o], rhpart.at[my], 0, o)
        to_rep(hnum, rhnum.at[my], 1, o)

    @pl.loop(1, n_own)
    def _(i):
        o = peer(i)
        to_owner(label.at[o], rlabel.at[me], 2, o)
        to_owner(bucket.at[0, o], rbucket.at[0, me], 3, o)

    pack(1)
    rbucket[1, me] = bucket[1, me]

    arrived(rhpart, 0, n_rep - 1)
    arrived(rhnum, 1, n_rep - 1)
    hsum = jnp.sum(rhpart[...], axis=0)
    num = jnp.sum(rhnum[...], axis=0)
    mine = iota((hot_rep, n_hot), 1) == iota((hot_rep, n_hot), 0) + my * hot_rep
    num = jnp.sum(jnp.where(mine, num, 0.0), axis=1, keepdims=True)
    num = jnp.broadcast_to(num, (hot_rep, LANES)).reshape(hot_rep, 1, LANES)
    for h in range(2):
        block = hsum[:, h * LANES : (h + 1) * LANES].reshape(hot_rep, 1, LANES)
        piece[h * hot_rep : (h + 1) * hot_rep, :, :LANES] = block
        piece[h * hot_rep : (h + 1) * hot_rep, :, LANES:] = num
    rpiece[me] = piece[me]

    @pl.loop(1, n_own)
    def _(i):
        o = peer(i)
        to_owner(piece.at[o], rpiece.at[me], 4, o)

    @pl.loop(1, n_own)
    def _(i):
        o = peer(i)
        to_owner(bucket.at[1, o], rbucket.at[1, me], 5, o)

    arrived(rlabel, 2, n_own - 1)
    per = LANES // CAP
    for j in range(n_own // per):
        wide[:, j * LANES : (j + 1) * LANES] = jnp.sum(rlabel[j * per : (j + 1) * per], axis=0)

    def add_up(h):
        high, lo = two_parts(rbucket[h].reshape(n_own * CAP, LANES))
        rhs[:, :LANES] = high
        rhs[:, LANES:] = lo

        def block(b):
            names = iota((per_rep, n_own * CAP), 0) + b * per_rep + 1
            hit = ones_where(names == wide[...]).astype(jnp.bfloat16)
            if h == 0:
                tally = dot(hit, jnp.ones((n_own * CAP, per_rep), jnp.bfloat16))
                return folded(dot(hit, rhs[...])), diagonal(tally)
            return folded(dot(hit, rhs[...])), None

        @pl.loop(0, n_rep - 1)
        def _(i):
            b = rep_peer(i)
            sums, tally = block(b)
            dense[h, b] = sums
            if h == 0:
                count[b] = tally

            @pl.when(i > 0)
            def _():
                o = rep_peer(i - 1)
                to_rep(dense.at[h, o], rdense.at[h, my], 6 + 2 * h, o)

        sums, tally = block(my)
        rdense[h, my] = sums
        if h == 0:
            rcount[my] = tally
        o = rep_peer(n_rep - 2)
        to_rep(dense.at[h, o], rdense.at[h, my], 6 + 2 * h, o)
        if h == 0:

            @pl.loop(0, n_rep - 1)
            def _(i):
                o = rep_peer(i)
                to_rep(count.at[o], rcount.at[my], 7, o)

    arrived(rbucket.at[0], 3, n_own - 1)
    add_up(0)

    arrived(rpiece, 4, n_own - 1)
    total = jnp.sum(rpiece[...], axis=0)
    done[:, :LANES] = total[:, :LANES] / jnp.sqrt(1.0 + total[:, LANES:])
    done[:, LANES:] = total[:, LANES:]
    rdone[me] = done[...]

    @pl.loop(1, n_own)
    def _(i):
        to_owner(done, rdone.at[me], 9, peer(i))

    arrived(rbucket.at[1], 5, n_own - 1)
    add_up(1)

    arrived(rdone, 9, n_own - 1)
    for h in range(2):
        block = rdone[h * hot_rep : (h + 1) * hot_rep, :, :LANES]
        hout[:, h * LANES : (h + 1) * LANES] = block.reshape(hot_rep, LANES)
    tally = rdone[:hot_rep, :, LANES : LANES + hot_rep].reshape(hot_rep, hot_rep)
    hcount[...] = diagonal(tally)

    arrived(rcount, 7, n_rep - 1)
    num = jnp.sum(rcount[...], axis=0)
    gcount[...] = num
    root = jnp.sqrt(1.0 + column(num))
    for h in range(2):
        arrived(rdense.at[h], 6 + 2 * h, n_rep - 1)
        gout[:, h * LANES : (h + 1) * LANES] = jnp.sum(rdense[h], axis=0) / root

    left(rhpart, 0, n_rep - 1)
    left(rhnum, 1, n_rep - 1)
    left(rlabel, 2, n_own - 1)
    left(rbucket.at[0], 3, n_own - 1)
    left(rpiece, 4, n_own - 1)
    left(rbucket.at[1], 5, n_own - 1)
    left(rdense.at[0], 6, n_rep - 1)
    left(rcount, 7, n_rep - 1)
    left(rdense.at[1], 8, n_rep - 1)
    left(rdone, 9, n_own - 1)


def local(n_own, n_rep, features, group_ids, survive, home_row, hot_ids):
    rows, width = features.shape
    groups, n_hot = home_row.shape[0], hot_ids.shape[0]
    own_groups = groups // n_own
    per_rep, hot_rep = own_groups // n_rep, n_hot // n_rep
    f32, i32 = jnp.float32, jnp.int32
    vmem = pl.BlockSpec(memory_space=pltpu.VMEM)
    hbm = pl.BlockSpec(memory_space=pl.ANY)
    gout, gcount, hout, hcount = pl.pallas_call(
        functools.partial(kernel, (n_own, n_rep, own_groups, n_hot)),
        out_shape=(
            jax.ShapeDtypeStruct((per_rep, width), f32),
            jax.ShapeDtypeStruct((1, per_rep), f32),
            jax.ShapeDtypeStruct((hot_rep, width), f32),
            jax.ShapeDtypeStruct((1, hot_rep), f32),
        ),
        in_specs=[vmem, vmem, vmem, hbm, hbm],
        out_specs=(vmem, vmem, vmem, vmem),
        scratch_shapes=[
            pltpu.VMEM((rows, width), f32),
            pltpu.VMEM((groups // LANES, LANES), i32),
            pltpu.VMEM((2, rows, 2 * LANES), jnp.bfloat16),
            pltpu.VMEM((2, n_own, CAP, LANES), f32),
            pltpu.VMEM((2, n_own, CAP, LANES), f32),
            pltpu.VMEM((n_own, 1, LANES), i32),
            pltpu.VMEM((n_own, 1, LANES), i32),
            pltpu.VMEM((1, n_own * CAP), i32),
            pltpu.VMEM((n_own * CAP, 2 * LANES), jnp.bfloat16),
            pltpu.VMEM((2, n_rep, per_rep, LANES), f32),
            pltpu.VMEM((2, n_rep, per_rep, LANES), f32),
            pltpu.VMEM((n_rep, 1, per_rep), f32),
            pltpu.VMEM((n_rep, 1, per_rep), f32),
            pltpu.VMEM((n_rep, hot_rep, width), f32),
            pltpu.VMEM((n_rep, hot_rep, width), f32),
            pltpu.VMEM((1, n_hot), f32),
            pltpu.VMEM((n_rep, 1, n_hot), f32),
            pltpu.VMEM((n_own, 1, 2 * LANES), f32),
            pltpu.VMEM((n_own, 1, 2 * LANES), f32),
            pltpu.VMEM((1, 2 * LANES), f32),
            pltpu.VMEM((n_own, 1, 2 * LANES), f32),
            pltpu.SemaphoreType.DMA((2,)),
            pltpu.SemaphoreType.DMA((10,)),
            pltpu.SemaphoreType.DMA((10,)),
        ],
        compiler_params=pltpu.CompilerParams(
            collective_id=0, has_side_effects=True, vmem_limit_bytes=32 * 1024 * 1024
        ),
    )(
        group_ids.reshape(1, rows),
        survive.reshape(1, rows),
        hot_ids.reshape(1, n_hot),
        features,
        home_row.reshape(groups // LANES, LANES),
    )
    return gout, gcount.reshape(per_rep), hout, hcount.reshape(hot_rep)


def solution(mesh):
    return jax.shard_map(
        functools.partial(local, mesh.shape["owner"], mesh.shape["rep"]),
        mesh=mesh,
        in_specs=(P(OWNER_REP, None), P(OWNER_REP), P(OWNER_REP), P(), P()),
        out_specs=(P(OWNER_REP, None), P(OWNER_REP), P("rep", None), P("rep")),
        check_vma=False,
    )
```

```python
import functools

import jax
import jax.numpy as jnp
from jax import lax
from jax.experimental import pallas as pl
from jax.experimental.pallas import tpu as pltpu
from jax.sharding import PartitionSpec as P

OWNER_REP = ("owner", "rep")
MESH = pl.DeviceIdType.MESH
LANES = 128
HALF = 64
CAP = 16
DEEP = 8
INNER = 8


def iota(shape, dim):
    return lax.broadcasted_iota(jnp.int32, shape, dim)


def ones_where(mask):
    return jnp.where(mask, 1.0, 0.0)


def two_parts(x):
    high = x.astype(jnp.bfloat16)
    low = (x - high.astype(jnp.float32)).astype(jnp.bfloat16)
    return high, low


def dot(a, b, dims=(((1,), (0,)), ((), ()))):
    return lax.dot_general(a, b, dims, preferred_element_type=jnp.float32)


def folded(x):
    return x[:, :LANES] + x[:, LANES:]


def column(row):
    n = row.shape[1]
    square = jnp.where(iota((n, n), 0) == iota((n, n), 1), row, 0.0)
    return jnp.sum(square, axis=1, keepdims=True)


def diagonal(square):
    n = square.shape[0]
    return jnp.sum(
        jnp.where(iota((n, n), 0) == iota((n, n), 1), square, 0.0), axis=0, keepdims=True
    )


def left_half(a, b):
    return jnp.where(iota(a.shape, 1) < HALF, a, b)


def turned(x):
    return pltpu.roll(x, HALF, 1)


def kernel(
    sizes,
    gid_hbm,
    live_hbm,
    hot_hbm,
    feat_hbm,
    home_hbm,
    gout,
    gcount,
    hout,
    hcount,
    gid_ref,
    live_ref,
    hot_ref,
    feat,
    home,
    parts,
    bucket,
    rbucket,
    label,
    rlabel,
    hits_of,
    rhs,
    dense,
    rdense,
    count,
    rcount,
    hpart,
    rhpart,
    hnum,
    rhnum,
    piece,
    rpiece,
    done,
    rdone,
    in_sem,
    send,
    recv,
):
    n_own, n_rep, own_groups, n_hot = sizes
    rows = gid_ref.shape[1]
    per_rep = own_groups // n_rep
    hot_rep = n_hot // n_rep
    n_z = n_own // INNER
    slots = n_own * DEEP
    me = lax.axis_index("owner")
    my = lax.axis_index("rep")
    zs = []
    for k in range(n_z):
        dz = ((k + 1) // 2) * (1 - 2 * (k % 2))
        zs.append(lax.rem(lax.div(me, INNER) + (dz + n_z), n_z) * INNER)
    x_me, c_me = lax.div(lax.rem(me, INNER), 2), lax.rem(me, 2)

    def each_owner(act):
        @pl.loop(0, INNER)
        def _(m):
            inner = lax.rem(x_me + lax.div(m, 2), INNER // 2) * 2 + lax.rem(c_me + m, 2)
            for k in range(n_z):
                if k == 0:

                    @pl.when(m > 0)
                    def _():
                        act(zs[0] + inner)
                else:
                    act(zs[k] + inner)

    def rep_at(step):
        return lax.rem(my + (step + n_rep), n_rep)

    copies = []
    for i, (src, dst) in enumerate(
        [
            (home_hbm, home),
            (gid_hbm, gid_ref),
            (live_hbm, live_ref),
            (hot_hbm, hot_ref),
            (feat_hbm, feat),
        ]
    ):
        copies.append(pltpu.make_async_copy(src, dst, in_sem.at[i]))
        copies[-1].start()

    barrier = pltpu.get_barrier_semaphore()

    def greet(o):
        pl.semaphore_signal(barrier, inc=1, device_id=(o, my), device_id_type=MESH)

    each_owner(greet)
    for step in range(1, n_rep):
        pl.semaphore_signal(barrier, inc=1, device_id=(me, rep_at(step)), device_id_type=MESH)

    for copy in copies[:4]:
        copy.wait()

    gid = gid_ref[...]
    live = live_ref[...] == 1
    match = iota((n_hot, n_hot), 0) == iota((n_hot, n_hot), 1)
    hot_ids = jnp.sum(
        jnp.where(match, hot_ref[...].astype(jnp.float32), 0.0), axis=1, keepdims=True
    )
    hits = ones_where(hot_ids == gid.astype(jnp.float32))
    is_hot = jnp.max(hits, axis=0, keepdims=True) > 0.5
    hot_table = jnp.where(live, hits, 0.0).astype(jnp.bfloat16)
    keep = jnp.logical_and(live, jnp.logical_not(is_hot))

    n_hi = home.shape[0]
    digits = jnp.concatenate(
        [
            (home[...] >> 8).astype(jnp.float32).astype(jnp.bfloat16),
            (home[...] & 255).astype(jnp.float32).astype(jnp.bfloat16),
        ],
        axis=1,
    )
    pick = ones_where(iota((n_hi, rows), 0) == (gid >> 7)).astype(jnp.bfloat16)
    found = dot(digits, pick, (((0,), (0,)), ((), ())))
    low = iota((LANES, rows), 0) == (gid & 127)
    d_high = jnp.sum(jnp.where(low, found[:LANES], 0.0), axis=0, keepdims=True)
    d_low = jnp.sum(jnp.where(low, found[LANES:], 0.0), axis=0, keepdims=True)
    dest = (d_high * 256.0 + d_low).astype(jnp.int32)
    owner = dest // own_groups
    local = dest % own_groups + 1
    member = ones_where(jnp.logical_and(iota((n_own, rows), 0) == owner, keep))
    before = ones_where(iota((rows, rows), 0) < iota((rows, rows), 1)).astype(jnp.bfloat16)
    earlier = dot(member.astype(jnp.bfloat16), before)
    pos = jnp.sum(member * earlier, axis=0, keepdims=True).astype(jnp.int32)
    deep = pos >= DEEP
    slot_a = jnp.where(jnp.logical_and(keep, jnp.logical_not(deep)), owner * DEEP + pos, -1)
    slot_b = jnp.where(jnp.logical_and(keep, deep), owner * DEEP + pos - DEEP, -1)

    shift = lax.rem(me, HALF // DEEP) * DEEP
    place = jnp.where(deep, pos + (HALF - DEEP), pos) + shift
    at = ones_where(iota((LANES, rows), 0) == place).astype(jnp.bfloat16)
    two = jnp.concatenate(
        [member * (local >> 5).astype(jnp.float32), member * (local & 31).astype(jnp.float32)],
        axis=0,
    ).astype(jnp.bfloat16)
    two = dot(two, at, (((1,), (1,)), ((), ())))
    names = (two[:n_own] * 32.0 + two[n_own:]).astype(jnp.int32)
    label[...] = names.reshape(n_own, 1, LANES)
    rlabel[me] = label[me]

    copies[4].wait()
    for t in range(2):
        block = feat[:, t * LANES : (t + 1) * LANES]
        for v in range(2):
            high, lo = two_parts(turned(block) if v else block)
            parts[t, v, :, :LANES] = high
            parts[t, v, :, LANES:] = lo

    tall = min(256, slots)

    def pack(t):
        @pl.loop(0, slots // tall)
        def _(j):
            lines = iota((tall, rows), 0) + j * tall
            a = folded(dot(ones_where(lines == slot_a).astype(jnp.bfloat16), parts[t, 0]))
            b = folded(dot(ones_where(lines == slot_b).astype(jnp.bfloat16), parts[t, 1]))
            to = pl.ds(j * (tall // DEEP), tall // DEEP)
            bucket[2 * t, to] = left_half(a, b).reshape(tall // DEEP, DEEP, LANES)
            bucket[2 * t + 1, to] = left_half(b, a).reshape(tall // DEEP, DEEP, LANES)

        for c in (2 * t, 2 * t + 1):
            rbucket[c, me] = bucket[c, me]

    def to_owner(src, dst, which, o):
        pltpu.make_async_remote_copy(
            src_ref=src,
            dst_ref=dst,
            send_sem=send.at[which],
            recv_sem=recv.at[which],
            device_id=(o, my),
            device_id_type=MESH,
        ).start()

    def to_rep(src, dst, which, o):
        pltpu.make_async_remote_copy(
            src_ref=src,
            dst_ref=dst,
            send_sem=send.at[which],
            recv_sem=recv.at[which],
            device_id=(me, o),
            device_id_type=MESH,
        ).start()

    def arrived(ref, which, n):
        pltpu.make_async_copy(ref.at[pl.ds(0, n)], ref.at[pl.ds(0, n)], recv.at[which]).wait()

    def left(ref, which, n):
        pltpu.make_async_copy(ref.at[pl.ds(0, n)], ref.at[pl.ds(0, n)], send.at[which]).wait()

    pack(0)
    pl.semaphore_wait(barrier, n_own - 1 + n_rep - 1)

    def send_first(o):
        to_owner(label.at[o], rlabel.at[me], 2, o)
        to_owner(bucket.at[0, o], rbucket.at[0, me], 3, o)

    each_owner(send_first)

    for t in range(2):
        part = folded(dot(hot_table, parts[t, 0]))
        hpart[:, :, t * LANES : (t + 1) * LANES] = part.reshape(n_rep, hot_rep, LANES)
    tally = dot(hot_table, jnp.ones((rows, n_hot), jnp.bfloat16))
    hnum[...] = diagonal(tally)
    rhpart[my] = hpart[my]
    rhnum[my] = hnum[...]
    pack(1)
    for step in range(1, n_rep):
        o = rep_at(step)
        to_rep(hpart.at[o], rhpart.at[my], 0, o)
        to_rep(hnum, rhnum.at[my], 1, o)
    for c in range(1, 4):
        each_owner(lambda o, c=c: to_owner(bucket.at[c, o], rbucket.at[c, me], 3 + c, o))

    arrived(rlabel, 2, n_own - 1)
    per = HALF // DEEP
    heaps = [jnp.sum(rlabel[j * per : (j + 1) * per], axis=0) for j in range(n_own // per)]
    if len(heaps) == 1:
        wide = [heaps[0][:, :HALF], heaps[0][:, HALF:]]
    else:
        wide = []
        for at_lane in (0, HALF):
            both = [h[:, at_lane : at_lane + HALF] for h in heaps]
            wide.append(jnp.concatenate(both, axis=1))

    @pl.loop(0, n_rep)
    def _(b):
        lines = iota((per_rep, slots), 0) + b * per_rep + 1
        for v in range(2):
            hit = ones_where(lines == wide[v]).astype(jnp.bfloat16)
            hits_of[b, v * per_rep : (v + 1) * per_rep] = hit
        tally = dot(hits_of[b], jnp.ones((slots, per_rep), jnp.bfloat16))
        count[b] = diagonal(tally[:per_rep] + tally[per_rep:])

    rcount[my] = count[my]
    for step in range(1, n_rep):
        o = rep_at(step)
        to_rep(count.at[o], rcount.at[my], 9, o)

    def add_up(c):
        arrived(rbucket.at[c], 3 + c, n_own - 1)
        high, lo = two_parts(rbucket[c].reshape(slots, LANES))
        rhs[:, :LANES] = high
        rhs[:, LANES:] = lo
        near = n_rep // 2

        def block(b):
            sums = folded(dot(hits_of[b], rhs[...]))
            a, z = sums[:per_rep], sums[per_rep:]
            if c % 2:
                a, z = z, a
            half = per_rep // 2
            straight = left_half(a[:half], z[half:])
            dense[c, b] = straight + turned(left_half(a[half:], z[:half]))

        def pair(j):
            return rep_at(j), lax.rem(my + n_rep - lax.rem(j, near), n_rep)

        def ship(j):
            a, b = pair(j)
            to_rep(dense.at[c, a], rdense.at[c, my], 10 + c, a)

            @pl.when(j < near)
            def _():
                to_rep(dense.at[c, b], rdense.at[c, my], 10 + c, b)

        @pl.loop(0, near)
        def _(i):
            a, b = pair(near - i)
            block(a)
            block(b)

            @pl.when(i > 0)
            def _():
                ship(near - i + 1)

        rdense[c, my] = dense[c, my]
        ship(1)

    add_up(0)

    arrived(rhpart, 0, n_rep - 1)
    arrived(rhnum, 1, n_rep - 1)
    hsum = jnp.sum(rhpart[...], axis=0)
    num = jnp.sum(rhnum[...], axis=0)
    mine = iota((hot_rep, n_hot), 1) == iota((hot_rep, n_hot), 0) + my * hot_rep
    num = jnp.sum(jnp.where(mine, num, 0.0), axis=1, keepdims=True)
    num = jnp.broadcast_to(num, (hot_rep, LANES)).reshape(hot_rep, 1, LANES)
    for h in range(2):
        block = hsum[:, h * LANES : (h + 1) * LANES].reshape(hot_rep, 1, LANES)
        piece[h * hot_rep : (h + 1) * hot_rep, :, :LANES] = block
        piece[h * hot_rep : (h + 1) * hot_rep, :, LANES:] = num
    rpiece[me] = piece[me]
    each_owner(lambda o: to_owner(piece.at[o], rpiece.at[me], 7, o))

    for c in range(1, 4):
        add_up(c)

    arrived(rpiece, 7, n_own - 1)
    total = jnp.sum(rpiece[...], axis=0)
    done[:, :LANES] = total[:, :LANES] / jnp.sqrt(1.0 + total[:, LANES:])
    done[:, LANES:] = total[:, LANES:]
    rdone[me] = done[...]
    each_owner(lambda o: to_owner(done, rdone.at[me], 8, o))

    arrived(rcount, 9, n_rep - 1)
    num = jnp.sum(rcount[...], axis=0)
    gcount[...] = num
    root = jnp.broadcast_to(jnp.sqrt(1.0 + column(num)), (per_rep, LANES))
    half = per_rep // 2
    root = left_half(root[:half], root[half:])

    def finish(t):
        whole = []
        for c in (2 * t, 2 * t + 1):
            arrived(rdense.at[c], 10 + c, n_rep - 1)
            whole.append(jnp.sum(rdense[c], axis=0) / root)
        a, b = whole
        gout[:half, t * LANES : (t + 1) * LANES] = left_half(a, turned(b))
        gout[half:, t * LANES : (t + 1) * LANES] = left_half(turned(a), b)

    finish(0)
    left(rhpart, 0, n_rep - 1)
    left(rhnum, 1, n_rep - 1)
    left(rlabel, 2, n_own - 1)
    for c in range(4):
        left(rbucket.at[c], 3 + c, n_own - 1)
    left(rpiece, 7, n_own - 1)

    arrived(rdone, 8, n_own - 1)
    for h in range(2):
        block = rdone[h * hot_rep : (h + 1) * hot_rep, :, :LANES]
        hout[:, h * LANES : (h + 1) * LANES] = block.reshape(hot_rep, LANES)
    tally = rdone[:hot_rep, :, LANES : LANES + hot_rep].reshape(hot_rep, hot_rep)
    hcount[...] = diagonal(tally)

    left(rdone, 8, n_own - 1)
    left(rcount, 9, n_rep - 1)
    finish(1)
    for c in range(4):
        left(rdense.at[c], 10 + c, n_rep - 1)


def write(*refs):
    sources, targets, sem = refs[:4], refs[4:8], refs[8]
    copies = [pltpu.make_async_copy(s, t, sem.at[i]) for i, (s, t) in enumerate(zip(sources, targets))]
    for copy in copies:
        copy.start()
    for copy in copies:
        copy.wait()


def local(n_own, n_rep, features, group_ids, survive, home_row, hot_ids):
    rows, width = features.shape
    groups, n_hot = home_row.shape[0], hot_ids.shape[0]
    own_groups = groups // n_own
    per_rep, hot_rep = own_groups // n_rep, n_hot // n_rep
    slots = n_own * DEEP
    f32, i32, bf16 = jnp.float32, jnp.int32, jnp.bfloat16
    vmem = pl.BlockSpec(memory_space=pltpu.VMEM)
    hbm = pl.BlockSpec(memory_space=pltpu.HBM)
    shapes = (
        jax.ShapeDtypeStruct((per_rep, width), f32),
        jax.ShapeDtypeStruct((1, per_rep), f32),
        jax.ShapeDtypeStruct((hot_rep, width), f32),
        jax.ShapeDtypeStruct((1, hot_rep), f32),
    )
    outs = pl.pallas_call(
        functools.partial(kernel, (n_own, n_rep, own_groups, n_hot)),
        out_shape=shapes,
        in_specs=[hbm] * 5,
        out_specs=(vmem,) * 4,
        scratch_shapes=[
            pltpu.VMEM((1, rows), i32),
            pltpu.VMEM((1, rows), i32),
            pltpu.VMEM((1, n_hot), i32),
            pltpu.VMEM((rows, width), f32),
            pltpu.VMEM((groups // LANES, LANES), i32),
            pltpu.VMEM((2, 2, rows, 2 * LANES), bf16),
            pltpu.VMEM((4, n_own, DEEP, LANES), f32),
            pltpu.VMEM((4, n_own, DEEP, LANES), f32),
            pltpu.VMEM((n_own, 1, LANES), i32),
            pltpu.VMEM((n_own, 1, LANES), i32),
            pltpu.VMEM((n_rep, 2 * per_rep, slots), bf16),
            pltpu.VMEM((slots, 2 * LANES), bf16),
            pltpu.VMEM((4, n_rep, per_rep // 2, LANES), f32),
            pltpu.VMEM((4, n_rep, per_rep // 2, LANES), f32),
            pltpu.VMEM((n_rep, 1, per_rep), f32),
            pltpu.VMEM((n_rep, 1, per_rep), f32),
            pltpu.VMEM((n_rep, hot_rep, width), f32),
            pltpu.VMEM((n_rep, hot_rep, width), f32),
            pltpu.VMEM((1, n_hot), f32),
            pltpu.VMEM((n_rep, 1, n_hot), f32),
            pltpu.VMEM((n_own, 1, 2 * LANES), f32),
            pltpu.VMEM((n_own, 1, 2 * LANES), f32),
            pltpu.VMEM((1, 2 * LANES), f32),
            pltpu.VMEM((n_own, 1, 2 * LANES), f32),
            pltpu.SemaphoreType.DMA((5,)),
            pltpu.SemaphoreType.DMA((14,)),
            pltpu.SemaphoreType.DMA((14,)),
        ],
        compiler_params=pltpu.CompilerParams(
            collective_id=0, has_side_effects=True, vmem_limit_bytes=67043328
        ),
    )(
        group_ids.reshape(1, rows),
        survive.reshape(1, rows),
        hot_ids.reshape(1, n_hot),
        features,
        home_row.reshape(groups // LANES, LANES),
    )
    gout, gcount, hout, hcount = pl.pallas_call(
        write,
        out_shape=shapes,
        in_specs=[vmem] * 4,
        out_specs=(hbm,) * 4,
        scratch_shapes=[pltpu.SemaphoreType.DMA((4,))],
    )(*outs)
    return gout, gcount.reshape(per_rep), hout, hcount.reshape(hot_rep)


def solution(mesh):
    return jax.shard_map(
        functools.partial(local, mesh.shape["owner"], mesh.shape["rep"]),
        mesh=mesh,
        in_specs=(P(OWNER_REP, None), P(OWNER_REP), P(OWNER_REP), P(), P()),
        out_specs=(P(OWNER_REP, None), P(OWNER_REP), P("rep", None), P("rep")),
        check_vma=False,
    )
```

```python
import functools

import jax
import jax.numpy as jnp
from jax import lax
from jax.experimental import pallas as pl
from jax.experimental.pallas import tpu as pltpu
from jax.sharding import PartitionSpec as P

OWNER_REP = ("owner", "rep")
MESH = pl.DeviceIdType.MESH
LANES = 128
CAP = 16
FOLD = 4
DEEP = CAP // FOLD
WIDE = LANES // FOLD
CHUNKS = 2 * FOLD
INNER = 8


CH = 6
RE = CH + CHUNKS


def iota(shape, dim):
    return lax.broadcasted_iota(jnp.int32, shape, dim)


def ones_where(mask):
    return jnp.where(mask, 1.0, 0.0)


def two_parts(x):
    high = x.astype(jnp.bfloat16)
    low = (x - high.astype(jnp.float32)).astype(jnp.bfloat16)
    return high, low


def dot(a, b, dims=(((1,), (0,)), ((), ()))):
    return lax.dot_general(a, b, dims, preferred_element_type=jnp.float32)


def folded(x):
    return x[:, :LANES] + x[:, LANES:]


def column(row):
    n = row.shape[1]
    square = jnp.where(iota((n, n), 0) == iota((n, n), 1), row, 0.0)
    return jnp.sum(square, axis=1, keepdims=True)


def diagonal(square):
    n = square.shape[0]
    return jnp.sum(
        jnp.where(iota((n, n), 0) == iota((n, n), 1), square, 0.0), axis=0, keepdims=True
    )


def woven(arrays):
    lane = iota(arrays[0].shape, 1)
    out = arrays[-1]
    for i in range(FOLD - 2, -1, -1):
        out = jnp.where(lane < (i + 1) * WIDE, arrays[i], out)
    return out


def turned(x, parts):
    parts %= FOLD
    return pltpu.roll(x, parts * WIDE, 1) if parts else x


def kernel(
    sizes,
    gid_hbm,
    live_hbm,
    hot_hbm,
    feat_hbm,
    home_hbm,
    gout,
    gcount,
    hout,
    hcount,
    gid_ref,
    live_ref,
    hot_ref,
    feat,
    home,
    parts,
    bucket,
    rbucket,
    label,
    rlabel,
    hits_of,
    rhs,
    dense,
    rdense,
    count,
    rcount,
    hpart,
    rhpart,
    hnum,
    rhnum,
    piece,
    rpiece,
    done,
    rdone,
    in_sem,
    send,
    recv,
):
    n_own, n_rep, own_groups, n_hot = sizes
    rows = gid_ref.shape[1]
    per_rep = own_groups // n_rep
    hot_rep = n_hot // n_rep
    n_z = n_own // INNER
    slots = n_own * DEEP
    me = lax.axis_index("owner")
    my = lax.axis_index("rep")
    z_me, x_me, c_me = lax.div(me, INNER), lax.div(lax.rem(me, INNER), 2), lax.rem(me, 2)
    inner = []
    for dx in (2, 1, 3, 0):
        for dc in (1, 0):
            inner.append(lax.rem(x_me + dx, INNER // 2) * 2 + lax.rem(c_me + dc, 2))

    def each_owner(act):
        @pl.loop(0, n_z)
        def _(k):
            far = n_z // 2 - lax.div(k + 1, 2)
            dz = far * (2 * lax.rem(k, 2) - 1)
            z = lax.rem(z_me + dz + n_z, n_z) * INNER
            for o in inner[:-1]:
                act(z + o)

            @pl.when(k < n_z - 1)
            def _():
                act(z + inner[-1])

    def rep_at(step):
        return lax.rem(my + (step + n_rep), n_rep)

    copies = []
    for i, (src, dst) in enumerate(
        [
            (home_hbm, home),
            (gid_hbm, gid_ref),
            (live_hbm, live_ref),
            (hot_hbm, hot_ref),
            (feat_hbm, feat),
        ]
    ):
        copies.append(pltpu.make_async_copy(src, dst, in_sem.at[i]))
        copies[-1].start()

    barrier = pltpu.get_barrier_semaphore()

    def greet(o):
        pl.semaphore_signal(barrier, inc=1, device_id=(o, my), device_id_type=MESH)

    each_owner(greet)
    for step in range(1, n_rep):
        pl.semaphore_signal(barrier, inc=1, device_id=(me, rep_at(step)), device_id_type=MESH)

    for copy in copies[:4]:
        copy.wait()

    gid = gid_ref[...]
    live = live_ref[...] == 1
    match = iota((n_hot, n_hot), 0) == iota((n_hot, n_hot), 1)
    hot_ids = jnp.sum(
        jnp.where(match, hot_ref[...].astype(jnp.float32), 0.0), axis=1, keepdims=True
    )
    hits = ones_where(hot_ids == gid.astype(jnp.float32))
    is_hot = jnp.max(hits, axis=0, keepdims=True) > 0.5
    hot_table = jnp.where(live, hits, 0.0).astype(jnp.bfloat16)
    keep = jnp.logical_and(live, jnp.logical_not(is_hot))

    n_hi = home.shape[0]
    digits = jnp.concatenate(
        [
            (home[...] >> 8).astype(jnp.float32).astype(jnp.bfloat16),
            (home[...] & 255).astype(jnp.float32).astype(jnp.bfloat16),
        ],
        axis=1,
    )
    pick = ones_where(iota((n_hi, rows), 0) == (gid >> 7)).astype(jnp.bfloat16)
    found = dot(digits, pick, (((0,), (0,)), ((), ())))
    low = iota((LANES, rows), 0) == (gid & 127)
    d_high = jnp.sum(jnp.where(low, found[:LANES], 0.0), axis=0, keepdims=True)
    d_low = jnp.sum(jnp.where(low, found[LANES:], 0.0), axis=0, keepdims=True)
    dest = (d_high * 256.0 + d_low).astype(jnp.int32)
    owner = dest // own_groups
    local = dest % own_groups + 1
    member = ones_where(jnp.logical_and(iota((n_own, rows), 0) == owner, keep))
    before = ones_where(iota((rows, rows), 0) < iota((rows, rows), 1)).astype(jnp.bfloat16)
    earlier = dot(member.astype(jnp.bfloat16), before)
    pos = jnp.sum(member * earlier, axis=0, keepdims=True).astype(jnp.int32)
    layer, depth = pos // DEEP, pos % DEEP
    slot = [
        jnp.where(jnp.logical_and(keep, layer == q), owner * DEEP + depth, -1) for q in range(FOLD)
    ]

    place = layer * WIDE + depth + lax.rem(me, WIDE // DEEP) * DEEP
    at = ones_where(iota((LANES, rows), 0) == place).astype(jnp.bfloat16)
    two = jnp.concatenate(
        [member * (local >> 5).astype(jnp.float32), member * (local & 31).astype(jnp.float32)],
        axis=0,
    ).astype(jnp.bfloat16)
    two = dot(two, at, (((1,), (1,)), ((), ())))
    names = (two[:n_own] * 32.0 + two[n_own:]).astype(jnp.int32)
    label[...] = names.reshape(n_own, 1, LANES)
    rlabel[me] = label[me]

    copies[4].wait()

    def pack(t):
        block = feat[:, t * LANES : (t + 1) * LANES]
        for q in range(FOLD):
            high, lo = two_parts(turned(block, q))
            parts[t, q, :, :LANES] = high
            parts[t, q, :, LANES:] = lo
        tall = min(128, slots)

        @pl.loop(0, slots // tall)
        def _(j):
            lines = iota((tall, rows), 0) + j * tall
            packed = []
            for q in range(FOLD):
                chosen = ones_where(lines == slot[q]).astype(jnp.bfloat16)
                packed.append(folded(dot(chosen, parts[t, q])))
            to = pl.ds(j * (tall // DEEP), tall // DEEP)
            for k in range(FOLD):
                message = woven([packed[(i - k) % FOLD] for i in range(FOLD)])
                bucket[t * FOLD + k, to] = message.reshape(tall // DEEP, DEEP, LANES)

        for k in range(FOLD):
            rbucket[t * FOLD + k, me] = bucket[t * FOLD + k, me]

    def to_owner(src, dst, which, o):
        pltpu.make_async_remote_copy(
            src_ref=src,
            dst_ref=dst,
            send_sem=send.at[which],
            recv_sem=recv.at[which],
            device_id=(o, my),
            device_id_type=MESH,
        ).start()

    def to_rep(src, dst, which, o):
        pltpu.make_async_remote_copy(
            src_ref=src,
            dst_ref=dst,
            send_sem=send.at[which],
            recv_sem=recv.at[which],
            device_id=(me, o),
            device_id_type=MESH,
        ).start()

    def arrived(ref, which, n):
        pltpu.make_async_copy(ref.at[pl.ds(0, n)], ref.at[pl.ds(0, n)], recv.at[which]).wait()

    def left(ref, which, n):
        pltpu.make_async_copy(ref.at[pl.ds(0, n)], ref.at[pl.ds(0, n)], send.at[which]).wait()

    pack(0)
    pl.semaphore_wait(barrier, n_own - 1 + n_rep - 1)

    each_owner(lambda o: to_owner(label.at[o], rlabel.at[me], 2, o))
    for c in range(2):
        each_owner(lambda o, c=c: to_owner(bucket.at[c, o], rbucket.at[c, me], CH + c, o))

    pack(1)
    for t in range(2):
        part = folded(dot(hot_table, parts[t, 0]))
        hpart[:, :, t * LANES : (t + 1) * LANES] = part.reshape(n_rep, hot_rep, LANES)
    tally = dot(hot_table, jnp.ones((rows, n_hot), jnp.bfloat16))
    hnum[...] = diagonal(tally)
    rhpart[my] = hpart[my]
    rhnum[my] = hnum[...]
    for step in range(1, n_rep):
        o = rep_at(step)
        to_rep(hpart.at[o], rhpart.at[my], 0, o)
        to_rep(hnum, rhnum.at[my], 1, o)
    for c in range(2, CHUNKS):
        each_owner(lambda o, c=c: to_owner(bucket.at[c, o], rbucket.at[c, me], CH + c, o))

    arrived(rlabel, 2, n_own - 1)
    per = WIDE // DEEP
    heaps = [jnp.sum(rlabel[j * per : (j + 1) * per], axis=0) for j in range(n_own // per)]
    wide = []
    for q in range(FOLD):
        some = [h[:, q * WIDE : (q + 1) * WIDE] for h in heaps]
        wide.append(some[0] if len(some) == 1 else jnp.concatenate(some, axis=1))

    @pl.loop(0, n_rep)
    def _(b):
        lines = iota((per_rep, slots), 0) + b * per_rep + 1
        for q in range(FOLD):
            hit = ones_where(lines == wide[q]).astype(jnp.bfloat16)
            hits_of[b, q * per_rep : (q + 1) * per_rep] = hit

    def count_up():
        @pl.loop(0, n_rep)
        def _(b):
            tally = dot(hits_of[b], jnp.ones((slots, per_rep), jnp.bfloat16))
            tally = sum(tally[q * per_rep : (q + 1) * per_rep] for q in range(FOLD))
            count[b] = diagonal(tally)

        rcount[my] = count[my]
        for step in range(1, n_rep):
            o = rep_at(step)
            to_rep(count.at[o], rcount.at[my], 5, o)

    def add_up(c):
        arrived(rbucket.at[c], CH + c, n_own - 1)
        high, lo = two_parts(rbucket[c].reshape(slots, LANES))
        rhs[:, :LANES] = high
        rhs[:, LANES:] = lo
        near = n_rep // 2

        def block(b):
            sums = folded(dot(hits_of[b], rhs[...]))
            low = per_rep // FOLD
            total = None
            for shift in range(FOLD):
                terms = []
                for i in range(FOLD):
                    start = ((i - c) % FOLD) * per_rep + ((i + shift) % FOLD) * low
                    terms.append(sums[start : start + low])
                term = turned(woven(terms), shift)
                total = term if total is None else total + term
            dense[c, b] = total

        def target(i):
            far = near - lax.div(i, 2)
            return lax.rem(my + n_rep + far * (1 - 2 * lax.rem(i, 2)), n_rep)

        def ship(i):
            o = target(i)
            to_rep(dense.at[c, o], rdense.at[c, my], RE + c, o)

        for i in range(1, n_rep):
            block(target(i))
        block(my)
        for i in range(1, n_rep):
            ship(i)
        rdense[c, my] = dense[c, my]

    add_up(0)
    count_up()
    add_up(1)

    arrived(rhpart, 0, n_rep - 1)
    arrived(rhnum, 1, n_rep - 1)
    hsum = jnp.sum(rhpart[...], axis=0)
    num = jnp.sum(rhnum[...], axis=0)
    mine = iota((hot_rep, n_hot), 1) == iota((hot_rep, n_hot), 0) + my * hot_rep
    num = jnp.sum(jnp.where(mine, num, 0.0), axis=1, keepdims=True)
    across = iota((hot_rep, LANES), 0) == iota((hot_rep, LANES), 1)
    num = jnp.sum(jnp.where(across, num, 0.0), axis=0, keepdims=True)
    piece[:, :, LANES:] = jnp.broadcast_to(num.reshape(1, 1, LANES), (n_own, 1, LANES))
    for h in range(2):
        block = hsum[:, h * LANES : (h + 1) * LANES].reshape(hot_rep, 1, LANES)
        piece[h * hot_rep : (h + 1) * hot_rep, :, :LANES] = block
    rpiece[me] = piece[me]
    each_owner(lambda o: to_owner(piece.at[o], rpiece.at[me], 3, o))

    for c in range(2, CHUNKS):
        add_up(c)

    arrived(rpiece, 3, n_own - 1)
    total = jnp.sum(rpiece[...], axis=0)
    done[...] = total[:, :LANES]
    hot_num = total[:, LANES:]
    rdone[me] = done[...]
    each_owner(lambda o: to_owner(done, rdone.at[me], 4, o))

    arrived(rcount, 5, n_rep - 1)
    num = jnp.sum(rcount[...], axis=0)
    gcount[...] = num
    root = jnp.broadcast_to(jnp.sqrt(1.0 + column(num)), (per_rep, LANES))
    low = per_rep // FOLD
    root = woven([root[g * low : (g + 1) * low] for g in range(FOLD)])

    def finish(t):
        whole = []
        for k in range(FOLD):
            c = t * FOLD + k
            arrived(rdense.at[c], RE + c, n_rep - 1)
            whole.append(jnp.sum(rdense[c], axis=0) / root)
        for g in range(FOLD):
            block = woven([turned(whole[k], k - g) for k in range(FOLD)])
            gout[g * low : (g + 1) * low, t * LANES : (t + 1) * LANES] = block

    finish(0)
    left(rhpart, 0, n_rep - 1)
    left(rhnum, 1, n_rep - 1)
    left(rlabel, 2, n_own - 1)
    for c in range(CHUNKS):
        left(rbucket.at[c], CH + c, n_own - 1)
    left(rpiece, 3, n_own - 1)

    arrived(rdone, 4, n_own - 1)
    hot_root = jnp.sum(jnp.where(across, hot_num, 0.0), axis=1, keepdims=True)
    hot_root = jnp.sqrt(1.0 + hot_root)
    for h in range(2):
        block = rdone[h * hot_rep : (h + 1) * hot_rep].reshape(hot_rep, LANES)
        hout[:, h * LANES : (h + 1) * LANES] = block / hot_root
    hcount[...] = hot_num[:, :hot_rep]

    left(rdone, 4, n_own - 1)
    left(rcount, 5, n_rep - 1)
    finish(1)
    for c in range(CHUNKS):
        left(rdense.at[c], RE + c, n_rep - 1)


def write(*refs):
    sources, targets, sem = refs[:4], refs[4:8], refs[8]
    copies = [pltpu.make_async_copy(s, t, sem.at[i]) for i, (s, t) in enumerate(zip(sources, targets))]
    for copy in copies:
        copy.start()
    for copy in copies:
        copy.wait()


def local(n_own, n_rep, features, group_ids, survive, home_row, hot_ids):
    rows, width = features.shape
    groups, n_hot = home_row.shape[0], hot_ids.shape[0]
    own_groups = groups // n_own
    per_rep, hot_rep = own_groups // n_rep, n_hot // n_rep
    slots = n_own * DEEP
    f32, i32, bf16 = jnp.float32, jnp.int32, jnp.bfloat16
    vmem = pl.BlockSpec(memory_space=pltpu.VMEM)
    hbm = pl.BlockSpec(memory_space=pltpu.HBM)
    shapes = (
        jax.ShapeDtypeStruct((per_rep, width), f32),
        jax.ShapeDtypeStruct((1, per_rep), f32),
        jax.ShapeDtypeStruct((hot_rep, width), f32),
        jax.ShapeDtypeStruct((1, hot_rep), f32),
    )
    outs = pl.pallas_call(
        functools.partial(kernel, (n_own, n_rep, own_groups, n_hot)),
        out_shape=shapes,
        in_specs=[hbm] * 5,
        out_specs=(vmem,) * 4,
        scratch_shapes=[
            pltpu.VMEM((1, rows), i32),
            pltpu.VMEM((1, rows), i32),
            pltpu.VMEM((1, n_hot), i32),
            pltpu.VMEM((rows, width), f32),
            pltpu.VMEM((groups // LANES, LANES), i32),
            pltpu.VMEM((2, FOLD, rows, 2 * LANES), bf16),
            pltpu.VMEM((CHUNKS, n_own, DEEP, LANES), f32),
            pltpu.VMEM((CHUNKS, n_own, DEEP, LANES), f32),
            pltpu.VMEM((n_own, 1, LANES), i32),
            pltpu.VMEM((n_own, 1, LANES), i32),
            pltpu.VMEM((n_rep, FOLD * per_rep, slots), bf16),
            pltpu.VMEM((slots, 2 * LANES), bf16),
            pltpu.VMEM((CHUNKS, n_rep, per_rep // FOLD, LANES), f32),
            pltpu.VMEM((CHUNKS, n_rep, per_rep // FOLD, LANES), f32),
            pltpu.VMEM((n_rep, 1, per_rep), f32),
            pltpu.VMEM((n_rep, 1, per_rep), f32),
            pltpu.VMEM((n_rep, hot_rep, width), f32),
            pltpu.VMEM((n_rep, hot_rep, width), f32),
            pltpu.VMEM((1, n_hot), f32),
            pltpu.VMEM((n_rep, 1, n_hot), f32),
            pltpu.VMEM((n_own, 1, 2 * LANES), f32),
            pltpu.VMEM((n_own, 1, 2 * LANES), f32),
            pltpu.VMEM((1, LANES), f32),
            pltpu.VMEM((n_own, 1, LANES), f32),
            pltpu.SemaphoreType.DMA((5,)),
            pltpu.SemaphoreType.DMA((RE + CHUNKS,)),
            pltpu.SemaphoreType.DMA((RE + CHUNKS,)),
        ],
        compiler_params=pltpu.CompilerParams(
            collective_id=0, has_side_effects=True, vmem_limit_bytes=67043328
        ),
    )(
        group_ids.reshape(1, rows),
        survive.reshape(1, rows),
        hot_ids.reshape(1, n_hot),
        features,
        home_row.reshape(groups // LANES, LANES),
    )
    gout, gcount, hout, hcount = pl.pallas_call(
        write,
        out_shape=shapes,
        in_specs=[vmem] * 4,
        out_specs=(hbm,) * 4,
        scratch_shapes=[pltpu.SemaphoreType.DMA((4,))],
    )(*outs)
    return gout, gcount.reshape(per_rep), hout, hcount.reshape(hot_rep)


def solution(mesh):
    return jax.shard_map(
        functools.partial(local, mesh.shape["owner"], mesh.shape["rep"]),
        mesh=mesh,
        in_specs=(P(OWNER_REP, None), P(OWNER_REP), P(OWNER_REP), P(), P()),
        out_specs=(P(OWNER_REP, None), P(OWNER_REP), P("rep", None), P("rep")),
        check_vma=False,
    )
```

```python
import functools

import jax
import jax.numpy as jnp
from jax import lax
from jax.experimental import pallas as pl
from jax.experimental.pallas import tpu as pltpu
from jax.sharding import PartitionSpec as P

OWNER_REP = ("owner", "rep")
MESH = pl.DeviceIdType.MESH
LANES = 128
CAP = 16
FOLD = 4
DEEP = CAP // FOLD
WIDE = LANES // FOLD
CHUNKS = 2 * FOLD
INNER = 8


CH = 6
RE = CH + CHUNKS


def iota(shape, dim):
    return lax.broadcasted_iota(jnp.int32, shape, dim)


def ones_where(mask):
    return jnp.where(mask, 1.0, 0.0)


def two_parts(x):
    high = x.astype(jnp.bfloat16)
    low = (x - high.astype(jnp.float32)).astype(jnp.bfloat16)
    return high, low


def dot(a, b, dims=(((1,), (0,)), ((), ()))):
    return lax.dot_general(a, b, dims, preferred_element_type=jnp.float32)


def folded(x):
    return x[:, :LANES] + x[:, LANES:]


def column(row):
    n = row.shape[1]
    square = jnp.where(iota((n, n), 0) == iota((n, n), 1), row, 0.0)
    return jnp.sum(square, axis=1, keepdims=True)


def diagonal(square):
    n = square.shape[0]
    return jnp.sum(
        jnp.where(iota((n, n), 0) == iota((n, n), 1), square, 0.0), axis=0, keepdims=True
    )


def woven(arrays):
    lane = iota(arrays[0].shape, 1)
    out = arrays[-1]
    for i in range(FOLD - 2, -1, -1):
        out = jnp.where(lane < (i + 1) * WIDE, arrays[i], out)
    return out


def turned(x, parts):
    parts %= FOLD
    return pltpu.roll(x, parts * WIDE, 1) if parts else x


def kernel(
    sizes,
    gid_hbm,
    live_hbm,
    hot_hbm,
    feat_hbm,
    home_hbm,
    gout,
    gcount,
    hout,
    hcount,
    gid_ref,
    live_ref,
    hot_ref,
    feat,
    home,
    parts,
    bucket,
    rbucket,
    label,
    rlabel,
    hits_of,
    rhs,
    dense,
    rdense,
    count,
    rcount,
    hpart,
    rhpart,
    hnum,
    rhnum,
    piece,
    rpiece,
    done,
    rdone,
    in_sem,
    send,
    recv,
):
    n_own, n_rep, own_groups, n_hot = sizes
    rows = gid_ref.shape[1]
    per_rep = own_groups // n_rep
    hot_rep = n_hot // n_rep
    n_z = n_own // INNER
    slots = n_own * DEEP
    me = lax.axis_index("owner")
    my = lax.axis_index("rep")
    z_me, x_me, c_me = lax.div(me, INNER), lax.div(lax.rem(me, INNER), 2), lax.rem(me, 2)
    inner = []
    for dx in (2, 1, 3, 0):
        for dc in (1, 0):
            inner.append(lax.rem(x_me + dx, INNER // 2) * 2 + lax.rem(c_me + dc, 2))

    def each_owner(act):
        @pl.loop(0, n_z)
        def _(k):
            far = n_z // 2 - lax.div(k + 1, 2)
            dz = far * (2 * lax.rem(k, 2) - 1)
            z = lax.rem(z_me + dz + n_z, n_z) * INNER
            for o in inner[:-1]:
                act(z + o)

            @pl.when(k < n_z - 1)
            def _():
                act(z + inner[-1])

    def rep_at(step):
        return lax.rem(my + (step + n_rep), n_rep)

    copies = []
    for i, (src, dst) in enumerate(
        [
            (home_hbm, home),
            (gid_hbm, gid_ref),
            (live_hbm, live_ref),
            (hot_hbm, hot_ref),
            (feat_hbm, feat),
        ]
    ):
        copies.append(pltpu.make_async_copy(src, dst, in_sem.at[i]))
        copies[-1].start()

    barrier = pltpu.get_barrier_semaphore()

    def greet(o):
        pl.semaphore_signal(barrier, inc=1, device_id=(o, my), device_id_type=MESH)

    each_owner(greet)
    for step in range(1, n_rep):
        pl.semaphore_signal(barrier, inc=1, device_id=(me, rep_at(step)), device_id_type=MESH)

    for copy in copies[:4]:
        copy.wait()

    gid = gid_ref[...]
    live = live_ref[...] == 1
    match = iota((n_hot, n_hot), 0) == iota((n_hot, n_hot), 1)
    hot_ids = jnp.sum(
        jnp.where(match, hot_ref[...].astype(jnp.float32), 0.0), axis=1, keepdims=True
    )
    hits = ones_where(hot_ids == gid.astype(jnp.float32))
    is_hot = jnp.max(hits, axis=0, keepdims=True) > 0.5
    hot_table = jnp.where(live, hits, 0.0).astype(jnp.bfloat16)
    keep = jnp.logical_and(live, jnp.logical_not(is_hot))

    n_hi = home.shape[0]
    digits = jnp.concatenate(
        [
            (home[...] >> 8).astype(jnp.float32).astype(jnp.bfloat16),
            (home[...] & 255).astype(jnp.float32).astype(jnp.bfloat16),
        ],
        axis=1,
    )
    pick = ones_where(iota((n_hi, rows), 0) == (gid >> 7)).astype(jnp.bfloat16)
    found = dot(digits, pick, (((0,), (0,)), ((), ())))
    low = iota((LANES, rows), 0) == (gid & 127)
    d_high = jnp.sum(jnp.where(low, found[:LANES], 0.0), axis=0, keepdims=True)
    d_low = jnp.sum(jnp.where(low, found[LANES:], 0.0), axis=0, keepdims=True)
    dest = (d_high * 256.0 + d_low).astype(jnp.int32)
    owner = dest // own_groups
    local = dest % own_groups + 1
    member = ones_where(jnp.logical_and(iota((n_own, rows), 0) == owner, keep))
    before = ones_where(iota((rows, rows), 0) < iota((rows, rows), 1)).astype(jnp.bfloat16)
    earlier = dot(member.astype(jnp.bfloat16), before)
    pos = jnp.sum(member * earlier, axis=0, keepdims=True).astype(jnp.int32)
    layer, depth = pos // DEEP, pos % DEEP
    slot = [
        jnp.where(jnp.logical_and(keep, layer == q), owner * DEEP + depth, -1) for q in range(FOLD)
    ]

    place = layer * WIDE + depth + lax.rem(me, WIDE // DEEP) * DEEP
    at = ones_where(iota((LANES, rows), 0) == place).astype(jnp.bfloat16)
    two = jnp.concatenate(
        [member * (local >> 5).astype(jnp.float32), member * (local & 31).astype(jnp.float32)],
        axis=0,
    ).astype(jnp.bfloat16)
    two = dot(two, at, (((1,), (1,)), ((), ())))
    names = (two[:n_own] * 32.0 + two[n_own:]).astype(jnp.int32)
    label[...] = names.reshape(n_own, 1, LANES)
    rlabel[me] = label[me]

    copies[4].wait()

    def pack(t):
        block = feat[:, t * LANES : (t + 1) * LANES]
        for q in range(FOLD):
            high, lo = two_parts(turned(block, q))
            parts[t, q, :, :LANES] = high
            parts[t, q, :, LANES:] = lo
        tall = min(128, slots)

        @pl.loop(0, slots // tall)
        def _(j):
            lines = iota((tall, rows), 0) + j * tall
            packed = []
            for q in range(FOLD):
                chosen = ones_where(lines == slot[q]).astype(jnp.bfloat16)
                packed.append(folded(dot(chosen, parts[t, q])))
            to = pl.ds(j * (tall // DEEP), tall // DEEP)
            for k in range(FOLD):
                message = woven([packed[(i - k) % FOLD] for i in range(FOLD)])
                bucket[t * FOLD + k, to] = message.reshape(tall // DEEP, DEEP, LANES)

        for k in range(FOLD):
            rbucket[t * FOLD + k, me] = bucket[t * FOLD + k, me]

    def to_owner(src, dst, which, o):
        pltpu.make_async_remote_copy(
            src_ref=src,
            dst_ref=dst,
            send_sem=send.at[which],
            recv_sem=recv.at[which],
            device_id=(o, my),
            device_id_type=MESH,
        ).start()

    def to_rep(src, dst, which, o):
        pltpu.make_async_remote_copy(
            src_ref=src,
            dst_ref=dst,
            send_sem=send.at[which],
            recv_sem=recv.at[which],
            device_id=(me, o),
            device_id_type=MESH,
        ).start()

    def arrived(ref, which, n):
        pltpu.make_async_copy(ref.at[pl.ds(0, n)], ref.at[pl.ds(0, n)], recv.at[which]).wait()

    def left(ref, which, n):
        pltpu.make_async_copy(ref.at[pl.ds(0, n)], ref.at[pl.ds(0, n)], send.at[which]).wait()

    pack(0)
    pl.semaphore_wait(barrier, n_own - 1 + n_rep - 1)

    each_owner(lambda o: to_owner(label.at[o], rlabel.at[me], 2, o))
    for c in range(2):
        each_owner(lambda o, c=c: to_owner(bucket.at[c, o], rbucket.at[c, me], CH + c, o))

    pack(1)
    for t in range(2):
        part = folded(dot(hot_table, parts[t, 0]))
        hpart[:, :, t * LANES : (t + 1) * LANES] = part.reshape(n_rep, hot_rep, LANES)
    tally = dot(hot_table, jnp.ones((rows, n_hot), jnp.bfloat16))
    hnum[...] = diagonal(tally)
    rhpart[my] = hpart[my]
    rhnum[my] = hnum[...]
    for step in range(1, n_rep):
        o = rep_at(step)
        to_rep(hpart.at[o], rhpart.at[my], 0, o)
        to_rep(hnum, rhnum.at[my], 1, o)
    for c in range(2, CHUNKS):
        each_owner(lambda o, c=c: to_owner(bucket.at[c, o], rbucket.at[c, me], CH + c, o))

    arrived(rlabel, 2, n_own - 1)
    per = WIDE // DEEP
    heaps = [jnp.sum(rlabel[j * per : (j + 1) * per], axis=0) for j in range(n_own // per)]
    wide = []
    for q in range(FOLD):
        some = [h[:, q * WIDE : (q + 1) * WIDE] for h in heaps]
        wide.append(some[0] if len(some) == 1 else jnp.concatenate(some, axis=1))

    @pl.loop(0, n_rep)
    def _(b):
        lines = iota((per_rep, slots), 0) + b * per_rep + 1
        for q in range(FOLD):
            hit = ones_where(lines == wide[q]).astype(jnp.bfloat16)
            hits_of[b, q * per_rep : (q + 1) * per_rep] = hit

    def count_up():
        @pl.loop(0, n_rep)
        def _(b):
            tally = dot(hits_of[b], jnp.ones((slots, per_rep), jnp.bfloat16))
            tally = sum(tally[q * per_rep : (q + 1) * per_rep] for q in range(FOLD))
            count[b] = diagonal(tally)

        rcount[my] = count[my]
        for step in range(1, n_rep):
            o = rep_at(step)
            to_rep(count.at[o], rcount.at[my], 5, o)

    def add_up(c):
        arrived(rbucket.at[c], CH + c, n_own - 1)
        high, lo = two_parts(rbucket[c].reshape(slots, LANES))
        rhs[:, :LANES] = high
        rhs[:, LANES:] = lo
        near = n_rep // 2

        def block(b):
            sums = folded(dot(hits_of[b], rhs[...]))
            low = per_rep // FOLD
            total = None
            for shift in range(FOLD):
                terms = []
                for i in range(FOLD):
                    start = ((i - c) % FOLD) * per_rep + ((i + shift) % FOLD) * low
                    terms.append(sums[start : start + low])
                term = turned(woven(terms), shift)
                total = term if total is None else total + term
            dense[c, b] = total

        def target(i):
            far = near - lax.div(i, 2)
            return lax.rem(my + n_rep + far * (1 - 2 * lax.rem(i, 2)), n_rep)

        def ship(i):
            o = target(i)
            to_rep(dense.at[c, o], rdense.at[c, my], RE + c, o)

        for i in range(1, n_rep):
            block(target(i))
        block(my)
        for i in range(1, n_rep):
            ship(i)
        rdense[c, my] = dense[c, my]

    add_up(0)
    count_up()
    add_up(1)

    arrived(rhpart, 0, n_rep - 1)
    arrived(rhnum, 1, n_rep - 1)
    hsum = jnp.sum(rhpart[...], axis=0)
    num = jnp.sum(rhnum[...], axis=0)
    mine = iota((hot_rep, n_hot), 1) == iota((hot_rep, n_hot), 0) + my * hot_rep
    num = jnp.sum(jnp.where(mine, num, 0.0), axis=1, keepdims=True)
    across = iota((hot_rep, LANES), 0) == iota((hot_rep, LANES), 1)
    num = jnp.sum(jnp.where(across, num, 0.0), axis=0, keepdims=True)
    piece[:, :, LANES:] = jnp.broadcast_to(num.reshape(1, 1, LANES), (n_own, 1, LANES))
    for h in range(2):
        block = hsum[:, h * LANES : (h + 1) * LANES].reshape(hot_rep, 1, LANES)
        piece[h * hot_rep : (h + 1) * hot_rep, :, :LANES] = block
    rpiece[me] = piece[me]
    each_owner(lambda o: to_owner(piece.at[o], rpiece.at[me], 3, o))

    for c in range(2, CHUNKS):
        add_up(c)

    arrived(rpiece, 3, n_own - 1)
    total = jnp.sum(rpiece[...], axis=0)
    done[...] = total[:, :LANES]
    hot_num = total[:, LANES:]
    rdone[me] = done[...]
    each_owner(lambda o: to_owner(done, rdone.at[me], 4, o))

    arrived(rcount, 5, n_rep - 1)
    num = jnp.sum(rcount[...], axis=0)
    gcount[...] = num
    root = jnp.broadcast_to(jnp.sqrt(1.0 + column(num)), (per_rep, LANES))
    low = per_rep // FOLD
    root = woven([root[g * low : (g + 1) * low] for g in range(FOLD)])

    def finish(t):
        whole = []
        for k in range(FOLD):
            c = t * FOLD + k
            arrived(rdense.at[c], RE + c, n_rep - 1)
            whole.append(jnp.sum(rdense[c], axis=0) / root)
        for g in range(FOLD):
            block = woven([turned(whole[k], k - g) for k in range(FOLD)])
            gout[g * low : (g + 1) * low, t * LANES : (t + 1) * LANES] = block

    finish(0)
    left(rhpart, 0, n_rep - 1)
    left(rhnum, 1, n_rep - 1)
    left(rlabel, 2, n_own - 1)
    for c in range(CHUNKS):
        left(rbucket.at[c], CH + c, n_own - 1)
    left(rpiece, 3, n_own - 1)

    arrived(rdone, 4, n_own - 1)
    hot_root = jnp.sum(jnp.where(across, hot_num, 0.0), axis=1, keepdims=True)
    hot_root = jnp.sqrt(1.0 + hot_root)
    for h in range(2):
        block = rdone[h * hot_rep : (h + 1) * hot_rep].reshape(hot_rep, LANES)
        hout[:, h * LANES : (h + 1) * LANES] = block / hot_root
    hcount[...] = hot_num[:, :hot_rep]

    left(rdone, 4, n_own - 1)
    left(rcount, 5, n_rep - 1)
    finish(1)
    for c in range(CHUNKS):
        left(rdense.at[c], RE + c, n_rep - 1)


def write(*refs):
    sources, targets, sem = refs[:4], refs[4:8], refs[8]
    copies = [pltpu.make_async_copy(s, t, sem.at[i]) for i, (s, t) in enumerate(zip(sources, targets))]
    for copy in copies:
        copy.start()
    for copy in copies:
        copy.wait()


def local(n_own, n_rep, features, group_ids, survive, home_row, hot_ids):
    rows, width = features.shape
    groups, n_hot = home_row.shape[0], hot_ids.shape[0]
    own_groups = groups // n_own
    per_rep, hot_rep = own_groups // n_rep, n_hot // n_rep
    slots = n_own * DEEP
    f32, i32, bf16 = jnp.float32, jnp.int32, jnp.bfloat16
    vmem = pl.BlockSpec(memory_space=pltpu.VMEM)
    hbm = pl.BlockSpec(memory_space=pltpu.HBM)
    shapes = (
        jax.ShapeDtypeStruct((per_rep, width), f32),
        jax.ShapeDtypeStruct((1, per_rep), f32),
        jax.ShapeDtypeStruct((hot_rep, width), f32),
        jax.ShapeDtypeStruct((1, hot_rep), f32),
    )
    given = (
        group_ids.reshape(1, rows),
        survive.reshape(1, rows),
        hot_ids.reshape(1, n_hot),
        features,
        home_row.reshape(groups // LANES, LANES),
    )
    outs = pl.pallas_call(
        functools.partial(kernel, (n_own, n_rep, own_groups, n_hot)),
        out_shape=tuple(pltpu.VMEM(s.shape, s.dtype) for s in shapes),
        in_specs=[hbm] * 5,
        out_specs=(vmem,) * 4,
        scratch_shapes=[
            pltpu.VMEM((1, rows), i32),
            pltpu.VMEM((1, rows), i32),
            pltpu.VMEM((1, n_hot), i32),
            pltpu.VMEM((rows, width), f32),
            pltpu.VMEM((groups // LANES, LANES), i32),
            pltpu.VMEM((2, FOLD, rows, 2 * LANES), bf16),
            pltpu.VMEM((CHUNKS, n_own, DEEP, LANES), f32),
            pltpu.VMEM((CHUNKS, n_own, DEEP, LANES), f32),
            pltpu.VMEM((n_own, 1, LANES), i32),
            pltpu.VMEM((n_own, 1, LANES), i32),
            pltpu.VMEM((n_rep, FOLD * per_rep, slots), bf16),
            pltpu.VMEM((slots, 2 * LANES), bf16),
            pltpu.VMEM((CHUNKS, n_rep, per_rep // FOLD, LANES), f32),
            pltpu.VMEM((CHUNKS, n_rep, per_rep // FOLD, LANES), f32),
            pltpu.VMEM((n_rep, 1, per_rep), f32),
            pltpu.VMEM((n_rep, 1, per_rep), f32),
            pltpu.VMEM((n_rep, hot_rep, width), f32),
            pltpu.VMEM((n_rep, hot_rep, width), f32),
            pltpu.VMEM((1, n_hot), f32),
            pltpu.VMEM((n_rep, 1, n_hot), f32),
            pltpu.VMEM((n_own, 1, 2 * LANES), f32),
            pltpu.VMEM((n_own, 1, 2 * LANES), f32),
            pltpu.VMEM((1, LANES), f32),
            pltpu.VMEM((n_own, 1, LANES), f32),
            pltpu.SemaphoreType.DMA((5,)),
            pltpu.SemaphoreType.DMA((RE + CHUNKS,)),
            pltpu.SemaphoreType.DMA((RE + CHUNKS,)),
        ],
        compiler_params=pltpu.CompilerParams(
            collective_id=0, has_side_effects=True, vmem_limit_bytes=32 * 1024 * 1024
        ),
    )(
        *(pltpu.with_memory_space_constraint(a, pltpu.HBM) for a in given)
    )
    gout, gcount, hout, hcount = pl.pallas_call(
        write,
        out_shape=shapes,
        in_specs=[vmem] * 4,
        out_specs=(hbm,) * 4,
        scratch_shapes=[pltpu.SemaphoreType.DMA((4,))],
        compiler_params=pltpu.CompilerParams(vmem_limit_bytes=1024 * 1024),
    )(*outs)
    return gout, gcount.reshape(per_rep), hout, hcount.reshape(hot_rep)


def solution(mesh):
    return jax.shard_map(
        functools.partial(local, mesh.shape["owner"], mesh.shape["rep"]),
        mesh=mesh,
        in_specs=(P(OWNER_REP, None), P(OWNER_REP), P(OWNER_REP), P(), P()),
        out_specs=(P(OWNER_REP, None), P(OWNER_REP), P("rep", None), P("rep")),
        check_vma=False,
    )
```

```python
import functools

import jax
import jax.numpy as jnp
from jax import lax
from jax.experimental import pallas as pl
from jax.experimental.pallas import tpu as pltpu
from jax.sharding import PartitionSpec as P

OWNER_REP = ("owner", "rep")
MESH = pl.DeviceIdType.MESH
LANES = 128
CAP = 16
FOLD = 4
DEEP = CAP // FOLD
WIDE = LANES // FOLD
CHUNKS = 2 * FOLD
INNER = 8


FIRST = 3
CH = 9
RE = CH + CHUNKS


def iota(shape, dim):
    return lax.broadcasted_iota(jnp.int32, shape, dim)


def ones_where(mask):
    return jnp.where(mask, 1.0, 0.0)


def two_parts(x):
    high = x.astype(jnp.bfloat16)
    low = (x - high.astype(jnp.float32)).astype(jnp.bfloat16)
    return high, low


def dot(a, b, dims=(((1,), (0,)), ((), ()))):
    return lax.dot_general(a, b, dims, preferred_element_type=jnp.float32)


def folded(x):
    return x[:, :LANES] + x[:, LANES:]


def column(row):
    n = row.shape[1]
    square = jnp.where(iota((n, n), 0) == iota((n, n), 1), row, 0.0)
    return jnp.sum(square, axis=1, keepdims=True)


def diagonal(square):
    n = square.shape[0]
    return jnp.sum(
        jnp.where(iota((n, n), 0) == iota((n, n), 1), square, 0.0), axis=0, keepdims=True
    )


def woven(arrays):
    lane = iota(arrays[0].shape, 1)
    out = arrays[-1]
    for i in range(FOLD - 2, -1, -1):
        out = jnp.where(lane < (i + 1) * WIDE, arrays[i], out)
    return out


def turned(x, parts):
    parts %= FOLD
    return pltpu.roll(x, parts * WIDE, 1) if parts else x


def kernel(
    sizes,
    gid_hbm,
    live_hbm,
    hot_hbm,
    feat_hbm,
    home_hbm,
    gout,
    gcount,
    hout,
    hcount,
    gid_ref,
    live_ref,
    hot_ref,
    feat,
    home,
    parts,
    bucket,
    rbucket,
    label,
    rlabel,
    hits_of,
    rhs,
    dense,
    rdense,
    count,
    rcount,
    hpart,
    rhpart,
    hnum,
    rhnum,
    piece,
    rpiece,
    rsome,
    level,
    rlevel,
    some_num,
    level_num,
    rlevel_num,
    done,
    rdone,
    in_sem,
    send,
    recv,
):
    n_own, n_rep, own_groups, n_hot = sizes
    rows = gid_ref.shape[1]
    per_rep = own_groups // n_rep
    hot_rep = n_hot // n_rep
    n_z = n_own // INNER
    slots = n_own * DEEP
    me = lax.axis_index("owner")
    my = lax.axis_index("rep")
    z_me, x_me, c_me = lax.div(me, INNER), lax.div(lax.rem(me, INNER), 2), lax.rem(me, 2)
    inner = []
    for dx in (2, 1, 3, 0):
        for dc in (1, 0):
            inner.append(lax.rem(x_me + dx, INNER // 2) * 2 + lax.rem(c_me + dc, 2))

    def each_owner(act):
        @pl.loop(0, n_z)
        def _(k):
            far = n_z // 2 - lax.div(k + 1, 2)
            dz = far * (2 * lax.rem(k, 2) - 1)
            z = lax.rem(z_me + dz + n_z, n_z) * INNER
            for o in inner[:-1]:
                act(z + o)

            @pl.when(k < n_z - 1)
            def _():
                act(z + inner[-1])

    def rep_at(step):
        return lax.rem(my + (step + n_rep), n_rep)

    copies = []
    for i, (src, dst) in enumerate(
        [
            (home_hbm, home),
            (gid_hbm, gid_ref),
            (live_hbm, live_ref),
            (hot_hbm, hot_ref),
            (feat_hbm, feat),
        ]
    ):
        copies.append(pltpu.make_async_copy(src, dst, in_sem.at[i]))
        copies[-1].start()

    barrier = pltpu.get_barrier_semaphore()

    def greet(o):
        pl.semaphore_signal(barrier, inc=1, device_id=(o, my), device_id_type=MESH)

    each_owner(greet)
    for step in range(1, n_rep):
        pl.semaphore_signal(barrier, inc=1, device_id=(me, rep_at(step)), device_id_type=MESH)

    for copy in copies[:4]:
        copy.wait()

    gid = gid_ref[...]
    live = live_ref[...] == 1
    match = iota((n_hot, n_hot), 0) == iota((n_hot, n_hot), 1)
    hot_ids = jnp.sum(
        jnp.where(match, hot_ref[...].astype(jnp.float32), 0.0), axis=1, keepdims=True
    )
    hits = ones_where(hot_ids == gid.astype(jnp.float32))
    is_hot = jnp.max(hits, axis=0, keepdims=True) > 0.5
    hot_table = jnp.where(live, hits, 0.0).astype(jnp.bfloat16)
    keep = jnp.logical_and(live, jnp.logical_not(is_hot))

    n_hi = home.shape[0]
    digits = jnp.concatenate(
        [
            (home[...] >> 8).astype(jnp.float32).astype(jnp.bfloat16),
            (home[...] & 255).astype(jnp.float32).astype(jnp.bfloat16),
        ],
        axis=1,
    )
    pick = ones_where(iota((n_hi, rows), 0) == (gid >> 7)).astype(jnp.bfloat16)
    found = dot(digits, pick, (((0,), (0,)), ((), ())))
    low = iota((LANES, rows), 0) == (gid & 127)
    d_high = jnp.sum(jnp.where(low, found[:LANES], 0.0), axis=0, keepdims=True)
    d_low = jnp.sum(jnp.where(low, found[LANES:], 0.0), axis=0, keepdims=True)
    dest = (d_high * 256.0 + d_low).astype(jnp.int32)
    owner = dest // own_groups
    local = dest % own_groups + 1
    member = ones_where(jnp.logical_and(iota((n_own, rows), 0) == owner, keep))
    before = ones_where(iota((rows, rows), 0) < iota((rows, rows), 1)).astype(jnp.bfloat16)
    earlier = dot(member.astype(jnp.bfloat16), before)
    pos = jnp.sum(member * earlier, axis=0, keepdims=True).astype(jnp.int32)
    layer, depth = pos // DEEP, pos % DEEP
    slot = [
        jnp.where(jnp.logical_and(keep, layer == q), owner * DEEP + depth, -1) for q in range(FOLD)
    ]

    place = layer * WIDE + depth + lax.rem(me, WIDE // DEEP) * DEEP
    at = ones_where(iota((LANES, rows), 0) == place).astype(jnp.bfloat16)
    two = jnp.concatenate(
        [member * (local >> 5).astype(jnp.float32), member * (local & 31).astype(jnp.float32)],
        axis=0,
    ).astype(jnp.bfloat16)
    two = dot(two, at, (((1,), (1,)), ((), ())))
    names = (two[:n_own] * 32.0 + two[n_own:]).astype(jnp.int32)
    label[...] = names.reshape(n_own, 1, LANES)
    rlabel[me] = label[me]

    copies[4].wait()

    def pack(t):
        block = feat[:, t * LANES : (t + 1) * LANES]
        for q in range(FOLD):
            high, lo = two_parts(turned(block, q))
            parts[t, q, :, :LANES] = high
            parts[t, q, :, LANES:] = lo
        tall = min(256, slots)

        @pl.loop(0, slots // tall)
        def _(j):
            lines = iota((tall, rows), 0) + j * tall
            packed = []
            for q in range(FOLD):
                chosen = ones_where(lines == slot[q]).astype(jnp.bfloat16)
                packed.append(folded(dot(chosen, parts[t, q])))
            to = pl.ds(j * (tall // DEEP), tall // DEEP)
            for k in range(FOLD):
                message = woven([packed[(i - k) % FOLD] for i in range(FOLD)])
                bucket[t * FOLD + k, to] = message.reshape(tall // DEEP, DEEP, LANES)

        for k in range(FOLD):
            rbucket[t * FOLD + k, me] = bucket[t * FOLD + k, me]

    def to_owner(src, dst, which, o):
        pltpu.make_async_remote_copy(
            src_ref=src,
            dst_ref=dst,
            send_sem=send.at[which],
            recv_sem=recv.at[which],
            device_id=(o, my),
            device_id_type=MESH,
        ).start()

    def to_rep(src, dst, which, o):
        pltpu.make_async_remote_copy(
            src_ref=src,
            dst_ref=dst,
            send_sem=send.at[which],
            recv_sem=recv.at[which],
            device_id=(me, o),
            device_id_type=MESH,
        ).start()

    def arrived(ref, which, n):
        pltpu.make_async_copy(ref.at[pl.ds(0, n)], ref.at[pl.ds(0, n)], recv.at[which]).wait()

    def left(ref, which, n):
        pltpu.make_async_copy(ref.at[pl.ds(0, n)], ref.at[pl.ds(0, n)], send.at[which]).wait()

    pack(0)
    pl.semaphore_wait(barrier, n_own - 1 + n_rep - 1)

    each_owner(lambda o: to_owner(label.at[o], rlabel.at[me], 2, o))
    for c in range(2):
        each_owner(lambda o, c=c: to_owner(bucket.at[c, o], rbucket.at[c, me], CH + c, o))

    pack(1)
    for t in range(2):
        part = folded(dot(hot_table, parts[t, 0]))
        hpart[:, :, t * LANES : (t + 1) * LANES] = part.reshape(n_rep, hot_rep, LANES)
    tally = dot(hot_table, jnp.ones((rows, n_hot), jnp.bfloat16))
    hnum[...] = diagonal(tally)
    rhpart[my] = hpart[my]
    rhnum[my] = hnum[...]
    for step in range(1, n_rep):
        o = rep_at(step)
        to_rep(hpart.at[o], rhpart.at[my], 0, o)
        to_rep(hnum, rhnum.at[my], 1, o)
    for c in range(2, CHUNKS):
        each_owner(lambda o, c=c: to_owner(bucket.at[c, o], rbucket.at[c, me], CH + c, o))

    arrived(rlabel, 2, n_own - 1)
    per = WIDE // DEEP
    heaps = [jnp.sum(rlabel[j * per : (j + 1) * per], axis=0) for j in range(n_own // per)]
    wide = []
    for q in range(FOLD):
        some = [h[:, q * WIDE : (q + 1) * WIDE] for h in heaps]
        wide.append(some[0] if len(some) == 1 else jnp.concatenate(some, axis=1))

    @pl.loop(0, n_rep)
    def _(b):
        lines = iota((per_rep, slots), 0) + b * per_rep + 1
        for q in range(FOLD):
            hit = ones_where(lines == wide[q]).astype(jnp.bfloat16)
            hits_of[b, q * per_rep : (q + 1) * per_rep] = hit

    def count_up():
        @pl.loop(0, n_rep)
        def _(b):
            tally = dot(hits_of[b], jnp.ones((slots, per_rep), jnp.bfloat16))
            tally = sum(tally[q * per_rep : (q + 1) * per_rep] for q in range(FOLD))
            count[b] = diagonal(tally)

        rcount[my] = count[my]
        for step in range(1, n_rep):
            o = rep_at(step)
            to_rep(count.at[o], rcount.at[my], 5, o)

    def add_up(c):
        arrived(rbucket.at[c], CH + c, n_own - 1)
        high, lo = two_parts(rbucket[c].reshape(slots, LANES))
        rhs[:, :LANES] = high
        rhs[:, LANES:] = lo
        near = n_rep // 2

        def block(b):
            sums = folded(dot(hits_of[b], rhs[...]))
            low = per_rep // FOLD
            total = None
            for shift in range(FOLD):
                terms = []
                for i in range(FOLD):
                    start = ((i - c) % FOLD) * per_rep + ((i + shift) % FOLD) * low
                    terms.append(sums[start : start + low])
                term = turned(woven(terms), shift)
                total = term if total is None else total + term
            dense[c, b] = total

        def target(i):
            far = near - lax.div(i, 2)
            return lax.rem(my + n_rep + far * (1 - 2 * lax.rem(i, 2)), n_rep)

        def ship(i):
            o = target(i)
            to_rep(dense.at[c, o], rdense.at[c, my], RE + c, o)

        for i in range(1, n_rep):
            block(target(i))
            if c == CHUNKS - 1 and i == FIRST:
                for k in range(1, FIRST + 1):
                    ship(k)
        block(my)
        for i in range(FIRST + 1 if c == CHUNKS - 1 and FIRST < n_rep else 1, n_rep):
            ship(i)
        rdense[c, my] = dense[c, my]

    add_up(0)
    count_up()
    add_up(1)

    arrived(rhpart, 0, n_rep - 1)
    arrived(rhnum, 1, n_rep - 1)
    hsum = jnp.sum(rhpart[...], axis=0)
    num = jnp.sum(rhnum[...], axis=0)
    mine = iota((hot_rep, n_hot), 1) == iota((hot_rep, n_hot), 0) + my * hot_rep
    num = jnp.sum(jnp.where(mine, num, 0.0), axis=1, keepdims=True)
    across = iota((hot_rep, LANES), 0) == iota((hot_rep, LANES), 1)
    some_num[...] = jnp.sum(jnp.where(across, num, 0.0), axis=0, keepdims=True)
    piece[...] = hsum.reshape(piece.shape)
    place = lax.rem(me, INNER)
    rpiece[place] = piece[place]
    rsome[place] = some_num[...]
    for o in inner[:-1]:
        to_owner(piece.at[o], rpiece.at[place], 3, z_me * INNER + o)
        to_owner(some_num, rsome.at[place], 4, z_me * INNER + o)

    add_up(2)
    add_up(3)

    arrived(rpiece, 3, INNER - 1)
    arrived(rsome, 4, INNER - 1)
    level[...] = jnp.sum(rpiece[...], axis=0)
    level_num[...] = jnp.sum(rsome[...], axis=0)
    rlevel[z_me] = level[...]
    rlevel_num[z_me] = level_num[...]
    for k in range(n_z - 1):
        far = n_z // 2 - (k + 1) // 2
        z = lax.rem(z_me + n_z + far * (2 * (k % 2) - 1), n_z)
        to_owner(level, rlevel.at[z_me], 6, z * INNER + place)
        to_owner(level_num, rlevel_num.at[z_me], 7, z * INNER + place)

    for c in range(4, CHUNKS):
        add_up(c)

    arrived(rlevel, 6, n_z - 1)
    arrived(rlevel_num, 7, n_z - 1)
    hot_num = jnp.sum(rlevel_num[...], axis=0)
    done[...] = jnp.sum(rlevel[...], axis=0)
    rdone[place] = done[...]
    for o in inner[:-1]:
        to_owner(done, rdone.at[place], 8, z_me * INNER + o)

    arrived(rcount, 5, n_rep - 1)
    num = jnp.sum(rcount[...], axis=0)
    gcount[...] = num
    root = jnp.broadcast_to(jnp.sqrt(1.0 + column(num)), (per_rep, LANES))
    low = per_rep // FOLD
    root = woven([root[g * low : (g + 1) * low] for g in range(FOLD)])

    def finish(t):
        whole = []
        for k in range(FOLD):
            c = t * FOLD + k
            arrived(rdense.at[c], RE + c, n_rep - 1)
            whole.append(jnp.sum(rdense[c], axis=0) / root)
        for g in range(FOLD):
            block = woven([turned(whole[k], k - g) for k in range(FOLD)])
            gout[g * low : (g + 1) * low, t * LANES : (t + 1) * LANES] = block

    finish(0)
    left(rhpart, 0, n_rep - 1)
    left(rhnum, 1, n_rep - 1)
    left(rlabel, 2, n_own - 1)
    for c in range(CHUNKS):
        left(rbucket.at[c], CH + c, n_own - 1)
    left(rpiece, 3, INNER - 1)
    left(rsome, 4, INNER - 1)
    left(rlevel, 6, n_z - 1)
    left(rlevel_num, 7, n_z - 1)

    arrived(rdone, 8, INNER - 1)
    hot_root = jnp.sum(jnp.where(across, hot_num, 0.0), axis=1, keepdims=True)
    hout[...] = rdone[...].reshape(hout.shape) / jnp.sqrt(1.0 + hot_root)
    hcount[...] = hot_num[:, :hot_rep]

    left(rdone, 8, INNER - 1)
    left(rcount, 5, n_rep - 1)
    finish(1)
    for c in range(CHUNKS):
        left(rdense.at[c], RE + c, n_rep - 1)


def write(*refs):
    sources, targets, sem = refs[:4], refs[4:8], refs[8]
    copies = [pltpu.make_async_copy(s, t, sem.at[i]) for i, (s, t) in enumerate(zip(sources, targets))]
    for copy in copies:
        copy.start()
    for copy in copies:
        copy.wait()


def local(n_own, n_rep, features, group_ids, survive, home_row, hot_ids):
    rows, width = features.shape
    groups, n_hot = home_row.shape[0], hot_ids.shape[0]
    own_groups = groups // n_own
    per_rep, hot_rep = own_groups // n_rep, n_hot // n_rep
    slots, share = n_own * DEEP, hot_rep // INNER
    f32, i32, bf16 = jnp.float32, jnp.int32, jnp.bfloat16
    vmem = pl.BlockSpec(memory_space=pltpu.VMEM)
    hbm = pl.BlockSpec(memory_space=pltpu.HBM)
    shapes = (
        jax.ShapeDtypeStruct((per_rep, width), f32),
        jax.ShapeDtypeStruct((1, per_rep), f32),
        jax.ShapeDtypeStruct((hot_rep, width), f32),
        jax.ShapeDtypeStruct((1, hot_rep), f32),
    )
    given = (
        group_ids.reshape(1, rows),
        survive.reshape(1, rows),
        hot_ids.reshape(1, n_hot),
        features,
        home_row.reshape(groups // LANES, LANES),
    )
    outs = pl.pallas_call(
        functools.partial(kernel, (n_own, n_rep, own_groups, n_hot)),
        out_shape=tuple(pltpu.VMEM(s.shape, s.dtype) for s in shapes),
        in_specs=[hbm] * 5,
        out_specs=(vmem,) * 4,
        scratch_shapes=[
            pltpu.VMEM((1, rows), i32),
            pltpu.VMEM((1, rows), i32),
            pltpu.VMEM((1, n_hot), i32),
            pltpu.VMEM((rows, width), f32),
            pltpu.VMEM((groups // LANES, LANES), i32),
            pltpu.VMEM((2, FOLD, rows, 2 * LANES), bf16),
            pltpu.VMEM((CHUNKS, n_own, DEEP, LANES), f32),
            pltpu.VMEM((CHUNKS, n_own, DEEP, LANES), f32),
            pltpu.VMEM((n_own, 1, LANES), i32),
            pltpu.VMEM((n_own, 1, LANES), i32),
            pltpu.VMEM((n_rep, FOLD * per_rep, slots), bf16),
            pltpu.VMEM((slots, 2 * LANES), bf16),
            pltpu.VMEM((CHUNKS, n_rep, per_rep // FOLD, LANES), f32),
            pltpu.VMEM((CHUNKS, n_rep, per_rep // FOLD, LANES), f32),
            pltpu.VMEM((n_rep, 1, per_rep), f32),
            pltpu.VMEM((n_rep, 1, per_rep), f32),
            pltpu.VMEM((n_rep, hot_rep, width), f32),
            pltpu.VMEM((n_rep, hot_rep, width), f32),
            pltpu.VMEM((1, n_hot), f32),
            pltpu.VMEM((n_rep, 1, n_hot), f32),
            pltpu.VMEM((INNER, share, width), f32),
            pltpu.VMEM((INNER, share, width), f32),
            pltpu.VMEM((INNER, 1, LANES), f32),
            pltpu.VMEM((share, width), f32),
            pltpu.VMEM((n_own // INNER, share, width), f32),
            pltpu.VMEM((1, LANES), f32),
            pltpu.VMEM((1, LANES), f32),
            pltpu.VMEM((n_own // INNER, 1, LANES), f32),
            pltpu.VMEM((share, width), f32),
            pltpu.VMEM((INNER, share, width), f32),
            pltpu.SemaphoreType.DMA((5,)),
            pltpu.SemaphoreType.DMA((RE + CHUNKS,)),
            pltpu.SemaphoreType.DMA((RE + CHUNKS,)),
        ],
        compiler_params=pltpu.CompilerParams(
            collective_id=0, has_side_effects=True, vmem_limit_bytes=32 * 1024 * 1024
        ),
    )(
        *(pltpu.with_memory_space_constraint(a, pltpu.HBM) for a in given)
    )
    gout, gcount, hout, hcount = pl.pallas_call(
        write,
        out_shape=shapes,
        in_specs=[vmem] * 4,
        out_specs=(hbm,) * 4,
        scratch_shapes=[pltpu.SemaphoreType.DMA((4,))],
        compiler_params=pltpu.CompilerParams(vmem_limit_bytes=1024 * 1024),
    )(*outs)
    return gout, gcount.reshape(per_rep), hout, hcount.reshape(hot_rep)


def solution(mesh):
    return jax.shard_map(
        functools.partial(local, mesh.shape["owner"], mesh.shape["rep"]),
        mesh=mesh,
        in_specs=(P(OWNER_REP, None), P(OWNER_REP), P(OWNER_REP), P(), P()),
        out_specs=(P(OWNER_REP, None), P(OWNER_REP), P("rep", None), P("rep")),
        check_vma=False,
    )
```

```python
import functools

import jax
import jax.numpy as jnp
from jax import lax
from jax.experimental import pallas as pl
from jax.experimental.pallas import tpu as pltpu
from jax.sharding import PartitionSpec as P

OWNER_REP = ("owner", "rep")
MESH = pl.DeviceIdType.MESH
LANES = 128
CAP = 16
FOLD = 4
DEEP = CAP // FOLD
WIDE = LANES // FOLD
CHUNKS = 2 * FOLD
INNER = 8


FIRST = 1
CH = 9
RE = CH + CHUNKS


def iota(shape, dim):
    return lax.broadcasted_iota(jnp.int32, shape, dim)


def ones_where(mask):
    return jnp.where(mask, 1.0, 0.0)


def two_parts(x):
    high = x.astype(jnp.bfloat16)
    low = (x - high.astype(jnp.float32)).astype(jnp.bfloat16)
    return high, low


def dot(a, b, dims=(((1,), (0,)), ((), ()))):
    return lax.dot_general(a, b, dims, preferred_element_type=jnp.float32)


def folded(x):
    return x[:, :LANES] + x[:, LANES:]


def column(row):
    n = row.shape[1]
    square = jnp.where(iota((n, n), 0) == iota((n, n), 1), row, 0.0)
    return jnp.sum(square, axis=1, keepdims=True)


def diagonal(square):
    n = square.shape[0]
    return jnp.sum(
        jnp.where(iota((n, n), 0) == iota((n, n), 1), square, 0.0), axis=0, keepdims=True
    )


def woven(arrays):
    lane = iota(arrays[0].shape, 1)
    out = arrays[-1]
    for i in range(FOLD - 2, -1, -1):
        out = jnp.where(lane < (i + 1) * WIDE, arrays[i], out)
    return out


def turned(x, parts):
    parts %= FOLD
    return pltpu.roll(x, parts * WIDE, 1) if parts else x


def kernel(
    sizes,
    gid_hbm,
    live_hbm,
    hot_hbm,
    feat_hbm,
    home_hbm,
    gout,
    gcount,
    hout,
    hcount,
    gid_ref,
    live_ref,
    hot_ref,
    feat,
    home,
    parts,
    bucket,
    rbucket,
    label,
    rlabel,
    hits_of,
    rhs,
    dense,
    rdense,
    count,
    rcount,
    hpart,
    rhpart,
    hnum,
    rhnum,
    piece,
    rpiece,
    rsome,
    level,
    rlevel,
    some_num,
    level_num,
    rlevel_num,
    done,
    rdone,
    in_sem,
    send,
    recv,
):
    n_own, n_rep, own_groups, n_hot = sizes
    rows = gid_ref.shape[1]
    per_rep = own_groups // n_rep
    hot_rep = n_hot // n_rep
    n_z = n_own // INNER
    slots = n_own * DEEP
    me = lax.axis_index("owner")
    my = lax.axis_index("rep")
    z_me, x_me, c_me = lax.div(me, INNER), lax.div(lax.rem(me, INNER), 2), lax.rem(me, 2)
    inner = []
    for dx in (2, 1, 3, 0):
        for dc in (1, 0):
            inner.append(lax.rem(x_me + dx, INNER // 2) * 2 + lax.rem(c_me + dc, 2))

    def each_owner(act):
        @pl.loop(0, n_z)
        def _(k):
            far = n_z // 2 - lax.div(k + 1, 2)
            dz = far * (2 * lax.rem(k, 2) - 1)
            z = lax.rem(z_me + dz + n_z, n_z) * INNER
            for o in inner[:-1]:
                act(z + o)

            @pl.when(k < n_z - 1)
            def _():
                act(z + inner[-1])

    def rep_at(step):
        return lax.rem(my + (step + n_rep), n_rep)

    copies = []
    for i, (src, dst) in enumerate(
        [
            (home_hbm, home),
            (gid_hbm, gid_ref),
            (live_hbm, live_ref),
            (hot_hbm, hot_ref),
            (feat_hbm, feat),
        ]
    ):
        copies.append(pltpu.make_async_copy(src, dst, in_sem.at[i]))
        copies[-1].start()

    barrier = pltpu.get_barrier_semaphore()

    def greet(o):
        pl.semaphore_signal(barrier, inc=1, device_id=(o, my), device_id_type=MESH)

    for k in range(n_z):
        far = n_z // 2 - (k + 1) // 2
        z = lax.rem(z_me + n_z + far * (2 * (k % 2) - 1), n_z) * INNER
        for o in inner if k < n_z - 1 else inner[:-1]:
            greet(z + o)
    for step in range(1, n_rep):
        pl.semaphore_signal(barrier, inc=1, device_id=(me, rep_at(step)), device_id_type=MESH)

    for copy in copies[:4]:
        copy.wait()

    gid = gid_ref[...]
    live = live_ref[...] == 1
    match = iota((n_hot, n_hot), 0) == iota((n_hot, n_hot), 1)
    hot_ids = jnp.sum(
        jnp.where(match, hot_ref[...].astype(jnp.float32), 0.0), axis=1, keepdims=True
    )
    hits = ones_where(hot_ids == gid.astype(jnp.float32))
    is_hot = jnp.max(hits, axis=0, keepdims=True) > 0.5
    hot_table = jnp.where(live, hits, 0.0).astype(jnp.bfloat16)
    keep = jnp.logical_and(live, jnp.logical_not(is_hot))

    n_hi = home.shape[0]
    digits = jnp.concatenate(
        [
            (home[...] >> 8).astype(jnp.float32).astype(jnp.bfloat16),
            (home[...] & 255).astype(jnp.float32).astype(jnp.bfloat16),
        ],
        axis=1,
    )
    pick = ones_where(iota((n_hi, rows), 0) == (gid >> 7)).astype(jnp.bfloat16)
    found = dot(digits, pick, (((0,), (0,)), ((), ())))
    low = iota((LANES, rows), 0) == (gid & 127)
    d_high = jnp.sum(jnp.where(low, found[:LANES], 0.0), axis=0, keepdims=True)
    d_low = jnp.sum(jnp.where(low, found[LANES:], 0.0), axis=0, keepdims=True)
    dest = (d_high * 256.0 + d_low).astype(jnp.int32)
    owner = dest // own_groups
    local = dest % own_groups + 1
    member = ones_where(jnp.logical_and(iota((n_own, rows), 0) == owner, keep))
    before = ones_where(iota((rows, rows), 0) < iota((rows, rows), 1)).astype(jnp.bfloat16)
    earlier = dot(member.astype(jnp.bfloat16), before)
    pos = jnp.sum(member * earlier, axis=0, keepdims=True).astype(jnp.int32)
    layer, depth = pos // DEEP, pos % DEEP
    slot = [
        jnp.where(jnp.logical_and(keep, layer == q), owner * DEEP + depth, -1) for q in range(FOLD)
    ]

    place = layer * WIDE + depth + lax.rem(me, WIDE // DEEP) * DEEP
    at = ones_where(iota((LANES, rows), 0) == place).astype(jnp.bfloat16)
    two = jnp.concatenate(
        [member * (local >> 5).astype(jnp.float32), member * (local & 31).astype(jnp.float32)],
        axis=0,
    ).astype(jnp.bfloat16)
    two = dot(two, at, (((1,), (1,)), ((), ())))
    names = (two[:n_own] * 32.0 + two[n_own:]).astype(jnp.int32)
    label[...] = names.reshape(n_own, 1, LANES)
    rlabel[me] = label[me]

    copies[4].wait()

    def pack(t):
        block = feat[:, t * LANES : (t + 1) * LANES]
        for q in range(FOLD):
            high, lo = two_parts(turned(block, q))
            parts[t, q, :, :LANES] = high
            parts[t, q, :, LANES:] = lo
        tall = min(256, slots)

        @pl.loop(0, slots // tall)
        def _(j):
            lines = iota((tall, rows), 0) + j * tall
            packed = []
            for q in range(FOLD):
                chosen = ones_where(lines == slot[q]).astype(jnp.bfloat16)
                packed.append(folded(dot(chosen, parts[t, q])))
            to = pl.ds(j * (tall // DEEP), tall // DEEP)
            for k in range(FOLD):
                message = woven([packed[(i - k) % FOLD] for i in range(FOLD)])
                bucket[t * FOLD + k, to] = message.reshape(tall // DEEP, DEEP, LANES)

        for k in range(FOLD):
            rbucket[t * FOLD + k, me] = bucket[t * FOLD + k, me]

    def to_owner(src, dst, which, o):
        pltpu.make_async_remote_copy(
            src_ref=src,
            dst_ref=dst,
            send_sem=send.at[which],
            recv_sem=recv.at[which],
            device_id=(o, my),
            device_id_type=MESH,
        ).start()

    def to_rep(src, dst, which, o):
        pltpu.make_async_remote_copy(
            src_ref=src,
            dst_ref=dst,
            send_sem=send.at[which],
            recv_sem=recv.at[which],
            device_id=(me, o),
            device_id_type=MESH,
        ).start()

    def arrived(ref, which, n):
        pltpu.make_async_copy(ref.at[pl.ds(0, n)], ref.at[pl.ds(0, n)], recv.at[which]).wait()

    def left(ref, which, n):
        pltpu.make_async_copy(ref.at[pl.ds(0, n)], ref.at[pl.ds(0, n)], send.at[which]).wait()

    pack(0)
    pl.semaphore_wait(barrier, n_own - 1 + n_rep - 1)

    each_owner(lambda o: to_owner(label.at[o], rlabel.at[me], 2, o))
    for c in range(2):
        each_owner(lambda o, c=c: to_owner(bucket.at[c, o], rbucket.at[c, me], CH + c, o))

    pack(1)
    for t in range(2):
        part = folded(dot(hot_table, parts[t, 0]))
        hpart[:, :, t * LANES : (t + 1) * LANES] = part.reshape(n_rep, hot_rep, LANES)
    tally = dot(hot_table, jnp.ones((rows, n_hot), jnp.bfloat16))
    hnum[...] = diagonal(tally)
    rhpart[my] = hpart[my]
    rhnum[my] = hnum[...]
    for step in range(1, n_rep):
        o = rep_at(step)
        to_rep(hpart.at[o], rhpart.at[my], 0, o)
        to_rep(hnum, rhnum.at[my], 1, o)
    for c in range(2, CHUNKS):
        each_owner(lambda o, c=c: to_owner(bucket.at[c, o], rbucket.at[c, me], CH + c, o))

    arrived(rlabel, 2, n_own - 1)
    per = WIDE // DEEP
    heaps = [jnp.sum(rlabel[j * per : (j + 1) * per], axis=0) for j in range(n_own // per)]
    wide = []
    for q in range(FOLD):
        some = [h[:, q * WIDE : (q + 1) * WIDE] for h in heaps]
        wide.append(some[0] if len(some) == 1 else jnp.concatenate(some, axis=1))

    @pl.loop(0, n_rep)
    def _(b):
        lines = iota((per_rep, slots), 0) + b * per_rep + 1
        for q in range(FOLD):
            hit = ones_where(lines == wide[q]).astype(jnp.bfloat16)
            hits_of[b, q * per_rep : (q + 1) * per_rep] = hit

    def count_up():
        @pl.loop(0, n_rep)
        def _(b):
            tally = dot(hits_of[b], jnp.ones((slots, per_rep), jnp.bfloat16))
            tally = sum(tally[q * per_rep : (q + 1) * per_rep] for q in range(FOLD))
            count[b] = diagonal(tally)

        rcount[my] = count[my]
        for step in range(1, n_rep):
            o = rep_at(step)
            to_rep(count.at[o], rcount.at[my], 5, o)

    def add_up(c):
        arrived(rbucket.at[c], CH + c, n_own - 1)
        high, lo = two_parts(rbucket[c].reshape(slots, LANES))
        rhs[:, :LANES] = high
        rhs[:, LANES:] = lo
        near = n_rep // 2

        def block(b):
            sums = folded(dot(hits_of[b], rhs[...]))
            low = per_rep // FOLD
            total = None
            for shift in range(FOLD):
                terms = []
                for i in range(FOLD):
                    start = ((i - c) % FOLD) * per_rep + ((i + shift) % FOLD) * low
                    terms.append(sums[start : start + low])
                term = turned(woven(terms), shift)
                total = term if total is None else total + term
            dense[c, b] = total

        def target(i):
            far = near - lax.div(i, 2)
            return lax.rem(my + n_rep + far * (1 - 2 * lax.rem(i, 2)), n_rep)

        def ship(i):
            o = target(i)
            to_rep(dense.at[c, o], rdense.at[c, my], RE + c, o)

        for i in range(1, n_rep):
            block(target(i))
            if c == CHUNKS - 1 and i == FIRST:
                for k in range(1, FIRST + 1):
                    ship(k)
        block(my)
        for i in range(FIRST + 1 if c == CHUNKS - 1 and FIRST < n_rep else 1, n_rep):
            ship(i)
        rdense[c, my] = dense[c, my]

    add_up(0)
    count_up()
    add_up(1)

    arrived(rhpart, 0, n_rep - 1)
    arrived(rhnum, 1, n_rep - 1)
    hsum = jnp.sum(rhpart[...], axis=0)
    num = jnp.sum(rhnum[...], axis=0)
    mine = iota((hot_rep, n_hot), 1) == iota((hot_rep, n_hot), 0) + my * hot_rep
    num = jnp.sum(jnp.where(mine, num, 0.0), axis=1, keepdims=True)
    across = iota((hot_rep, LANES), 0) == iota((hot_rep, LANES), 1)
    some_num[...] = jnp.sum(jnp.where(across, num, 0.0), axis=0, keepdims=True)
    piece[...] = hsum.reshape(piece.shape)
    place = lax.rem(me, INNER)
    rpiece[place] = piece[place]
    rsome[place] = some_num[...]
    for o in inner[:-1]:
        to_owner(piece.at[o], rpiece.at[place], 3, z_me * INNER + o)
        to_owner(some_num, rsome.at[place], 4, z_me * INNER + o)

    add_up(2)
    add_up(3)

    arrived(rpiece, 3, INNER - 1)
    arrived(rsome, 4, INNER - 1)
    level[...] = jnp.sum(rpiece[...], axis=0)
    level_num[...] = jnp.sum(rsome[...], axis=0)
    rlevel[z_me] = level[...]
    rlevel_num[z_me] = level_num[...]
    for k in range(n_z - 1):
        far = n_z // 2 - (k + 1) // 2
        z = lax.rem(z_me + n_z + far * (2 * (k % 2) - 1), n_z)
        to_owner(level, rlevel.at[z_me], 6, z * INNER + place)
        to_owner(level_num, rlevel_num.at[z_me], 7, z * INNER + place)

    for c in range(4, CHUNKS):
        add_up(c)

    arrived(rlevel, 6, n_z - 1)
    arrived(rlevel_num, 7, n_z - 1)
    hot_num = jnp.sum(rlevel_num[...], axis=0)
    done[...] = jnp.sum(rlevel[...], axis=0)
    rdone[place] = done[...]
    for o in inner[:-1]:
        to_owner(done, rdone.at[place], 8, z_me * INNER + o)

    arrived(rcount, 5, n_rep - 1)
    num = jnp.sum(rcount[...], axis=0)
    gcount[...] = num
    root = jnp.broadcast_to(jnp.sqrt(1.0 + column(num)), (per_rep, LANES))
    low = per_rep // FOLD
    root = woven([root[g * low : (g + 1) * low] for g in range(FOLD)])

    def finish(t):
        whole = []
        for k in range(FOLD):
            c = t * FOLD + k
            arrived(rdense.at[c], RE + c, n_rep - 1)
            whole.append(jnp.sum(rdense[c], axis=0) / root)
        for g in range(FOLD):
            block = woven([turned(whole[k], k - g) for k in range(FOLD)])
            gout[g * low : (g + 1) * low, t * LANES : (t + 1) * LANES] = block

    finish(0)
    left(rhpart, 0, n_rep - 1)
    left(rhnum, 1, n_rep - 1)
    left(rlabel, 2, n_own - 1)
    for c in range(CHUNKS):
        left(rbucket.at[c], CH + c, n_own - 1)
    left(rpiece, 3, INNER - 1)
    left(rsome, 4, INNER - 1)
    left(rlevel, 6, n_z - 1)
    left(rlevel_num, 7, n_z - 1)

    arrived(rdone, 8, INNER - 1)
    hot_root = jnp.sum(jnp.where(across, hot_num, 0.0), axis=1, keepdims=True)
    hout[...] = rdone[...].reshape(hout.shape) / jnp.sqrt(1.0 + hot_root)
    hcount[...] = hot_num[:, :hot_rep]

    left(rdone, 8, INNER - 1)
    left(rcount, 5, n_rep - 1)
    finish(1)
    for c in range(CHUNKS):
        left(rdense.at[c], RE + c, n_rep - 1)


def write(*refs):
    sources, targets, sem = refs[:4], refs[4:8], refs[8]
    copies = [pltpu.make_async_copy(s, t, sem.at[i]) for i, (s, t) in enumerate(zip(sources, targets))]
    for copy in copies:
        copy.start()
    for copy in copies:
        copy.wait()


def local(n_own, n_rep, features, group_ids, survive, home_row, hot_ids):
    rows, width = features.shape
    groups, n_hot = home_row.shape[0], hot_ids.shape[0]
    own_groups = groups // n_own
    per_rep, hot_rep = own_groups // n_rep, n_hot // n_rep
    slots, share = n_own * DEEP, hot_rep // INNER
    f32, i32, bf16 = jnp.float32, jnp.int32, jnp.bfloat16
    vmem = pl.BlockSpec(memory_space=pltpu.VMEM)
    hbm = pl.BlockSpec(memory_space=pltpu.HBM)
    shapes = (
        jax.ShapeDtypeStruct((per_rep, width), f32),
        jax.ShapeDtypeStruct((1, per_rep), f32),
        jax.ShapeDtypeStruct((hot_rep, width), f32),
        jax.ShapeDtypeStruct((1, hot_rep), f32),
    )
    given = (
        group_ids.reshape(1, rows),
        survive.reshape(1, rows),
        hot_ids.reshape(1, n_hot),
        features,
        home_row.reshape(groups // LANES, LANES),
    )
    outs = pl.pallas_call(
        functools.partial(kernel, (n_own, n_rep, own_groups, n_hot)),
        out_shape=tuple(pltpu.VMEM(s.shape, s.dtype) for s in shapes),
        in_specs=[hbm] * 5,
        out_specs=(vmem,) * 4,
        scratch_shapes=[
            pltpu.VMEM((1, rows), i32),
            pltpu.VMEM((1, rows), i32),
            pltpu.VMEM((1, n_hot), i32),
            pltpu.VMEM((rows, width), f32),
            pltpu.VMEM((groups // LANES, LANES), i32),
            pltpu.VMEM((2, FOLD, rows, 2 * LANES), bf16),
            pltpu.VMEM((CHUNKS, n_own, DEEP, LANES), f32),
            pltpu.VMEM((CHUNKS, n_own, DEEP, LANES), f32),
            pltpu.VMEM((n_own, 1, LANES), i32),
            pltpu.VMEM((n_own, 1, LANES), i32),
            pltpu.VMEM((n_rep, FOLD * per_rep, slots), bf16),
            pltpu.VMEM((slots, 2 * LANES), bf16),
            pltpu.VMEM((CHUNKS, n_rep, per_rep // FOLD, LANES), f32),
            pltpu.VMEM((CHUNKS, n_rep, per_rep // FOLD, LANES), f32),
            pltpu.VMEM((n_rep, 1, per_rep), f32),
            pltpu.VMEM((n_rep, 1, per_rep), f32),
            pltpu.VMEM((n_rep, hot_rep, width), f32),
            pltpu.VMEM((n_rep, hot_rep, width), f32),
            pltpu.VMEM((1, n_hot), f32),
            pltpu.VMEM((n_rep, 1, n_hot), f32),
            pltpu.VMEM((INNER, share, width), f32),
            pltpu.VMEM((INNER, share, width), f32),
            pltpu.VMEM((INNER, 1, LANES), f32),
            pltpu.VMEM((share, width), f32),
            pltpu.VMEM((n_own // INNER, share, width), f32),
            pltpu.VMEM((1, LANES), f32),
            pltpu.VMEM((1, LANES), f32),
            pltpu.VMEM((n_own // INNER, 1, LANES), f32),
            pltpu.VMEM((share, width), f32),
            pltpu.VMEM((INNER, share, width), f32),
            pltpu.SemaphoreType.DMA((5,)),
            pltpu.SemaphoreType.DMA((RE + CHUNKS,)),
            pltpu.SemaphoreType.DMA((RE + CHUNKS,)),
        ],
        compiler_params=pltpu.CompilerParams(
            collective_id=0, has_side_effects=True, vmem_limit_bytes=32 * 1024 * 1024
        ),
    )(
        *(pltpu.with_memory_space_constraint(a, pltpu.HBM) for a in given)
    )
    gout, gcount, hout, hcount = pl.pallas_call(
        write,
        out_shape=shapes,
        in_specs=[vmem] * 4,
        out_specs=(hbm,) * 4,
        scratch_shapes=[pltpu.SemaphoreType.DMA((4,))],
        compiler_params=pltpu.CompilerParams(vmem_limit_bytes=1024 * 1024),
    )(*outs)
    return gout, gcount.reshape(per_rep), hout, hcount.reshape(hot_rep)


def solution(mesh):
    return jax.shard_map(
        functools.partial(local, mesh.shape["owner"], mesh.shape["rep"]),
        mesh=mesh,
        in_specs=(P(OWNER_REP, None), P(OWNER_REP), P(OWNER_REP), P(), P()),
        out_specs=(P(OWNER_REP, None), P(OWNER_REP), P("rep", None), P("rep")),
        check_vma=False,
    )
```
